128 devices in a mesh: tm: 32 (over z_hi, y, x), freq: 4 (over z_lo, core).
Axes of the slice: x: 4, y: 4, z: 4 (z_hi: 2, z_lo: 2; z = z_hi * 2 + z_lo), core: 2. Of those that a mesh axis runs over, the one named last changes fastest.
Arguments:
- sfts: float32 [1536, 2, 4096], P('tm', None, 'freq'), may hold values from -40 to 40
- detector_ids: int32 [1536], replicated, may hold values from 0 to 2
- intersection: float32 [3, 3], replicated, may hold values from 0.3 to 1
- lags: int32 [12], replicated, may hold values from 1 to 16, as said below
- template_ids: int32 [4096, 2], P('tm'), may hold values from 0 to 63
Outputs:
- stat: float32 [4096, 4096], P('tm', 'freq')
The draws below stay inside these ranges and needn't reach their ends.
Inputs may be any that keep to these rules, and one draw needn't show every extreme that they name: 12 distinct lags, one of them 16.
All inputs are finite; a program needn't handle non-finite values.
Results may differ from the reference program's by a relative error of at most 0.009.
Values may be sent and summed in bfloat16 or wider, within the bound.
No kernel may reach another device: no remote copies, remote signals or barrier semaphores. Data moves between devices by JAX's collectives and lax.ppermute only.
A program may use at most 64 MiB of HBM per device.

```python
import math
import jax
import jax.numpy as jnp
from jax import lax

NBIN = 4096
NTEMPL = 4096
LAGMAX = 16
NLAG = 12
NDET = 3
NGRID = 64
PERIOD = 283
SFT_DEV = 48
NSFT = 1536


def draw_sfts(key, part):
    key_base = jax.random.fold_in(key, 11)
    key_rough = jax.random.fold_in(key, 12)
    key_rows = jax.random.fold_in(key, 13)
    bins = jnp.arange(NBIN, dtype=jnp.float32)
    ramp = jnp.exp(0.55 * bins / NBIN)
    rough = jax.random.uniform(key_rough, (NBIN,), jnp.float32, 0.6, 1.4)
    base = jnp.clip(jax.random.normal(key_base, (NSFT, 2, NBIN), jnp.float32), -6.0, 6.0)
    row_scale = jnp.exp(jax.random.uniform(key_rows, (NSFT,), jnp.float32, math.log(0.5), math.log(2.0)))
    values = base * row_scale[:, None, None] * (ramp * rough)[None, None, :]
    return jnp.clip(values, -40.0, 40.0).astype(jnp.float32)


def draw_lags(key, part):
    order = jax.random.permutation(jax.random.fold_in(key, 21), LAGMAX - 1)[:NLAG - 1].astype(jnp.int32) + 1
    return jnp.concatenate([jnp.full((1,), LAGMAX, jnp.int32), order])


def place_ends(array, stream_key, least, largest):
    longest = array.shape.index(max(array.shape))
    spots = []
    for shift in (0, 1):
        where = [jax.random.randint(jax.random.fold_in(stream_key, axis), (), 0, length) for axis, length in enumerate(array.shape)]
        where[longest] = (where[longest] + shift) % array.shape[longest]
        spots.append(tuple(where))
    return array.at[spots[0]].set(least).at[spots[1]].set(largest)


def setup_inputs(seed: int = 0) -> dict:
    key_list = jax.random.split(jax.random.key(seed), 6)
    sfts = draw_sfts(jax.random.fold_in(key_list[5], 71), 0)
    detector_ids = place_ends(jax.random.randint(key_list[1], (NSFT,), 0, NDET), jax.random.fold_in(key_list[1], 1), 0, NDET - 1).astype(jnp.int32)
    intersection = jnp.clip(jax.random.uniform(key_list[2], (NDET, NDET), jnp.float32, 0.3, 1.0), 0.3, 1.0)
    lags = draw_lags(jax.random.fold_in(key_list[5], 71), 0)
    template_ids = place_ends(jax.random.randint(key_list[4], (NTEMPL, 2), 0, NGRID), jax.random.fold_in(key_list[4], 1), 0, NGRID - 1).astype(jnp.int32)
    return {"sfts": sfts, "detector_ids": detector_ids, "intersection": intersection, "lags": lags, "template_ids": template_ids}


def block_term(extended, first_row, ids_padded, lag_list, intersection, amplitude_idx, phase_idx, total):
    span = extended.shape[0] - LAGMAX
    here = jnp.arange(span, dtype=jnp.int32)
    partner = here[None, :] + lag_list[:, None]
    own_rows = extended[:span].astype(jnp.float32)
    far_rows = extended[partner].astype(jnp.float32)
    det_block = lax.dynamic_slice_in_dim(ids_padded, first_row, extended.shape[0], 0)
    det_near = det_block[:span]
    det_far = det_block[partner]
    levels = jnp.arange(intersection.shape[0], dtype=jnp.int32)
    hot_near = (det_near[:, None] == levels[None, :]).astype(jnp.float32)
    hot_far = (det_far[:, :, None] == levels[None, None, :]).astype(jnp.float32)
    weight = jnp.einsum('sa,ab,lsb->ls', hot_near, intersection.astype(jnp.float32), hot_far)
    inside = first_row + partner < total
    weight = jnp.where(inside, weight, jnp.float32(0.0))
    re_own = own_rows[None, :, 0]
    im_own = own_rows[None, :, 1]
    re_far = far_rows[:, :, 0]
    im_far = far_rows[:, :, 1]
    pair_re = (weight[:, :, None] * (re_own * re_far + im_own * im_far)).astype(jnp.bfloat16)
    pair_im = (weight[:, :, None] * (re_own * im_far - im_own * re_far)).astype(jnp.bfloat16)
    width = extended.shape[2]
    stacked = jnp.concatenate([pair_re.reshape(-1, width), pair_im.reshape(-1, width)], 0)
    position = first_row + jnp.arange(extended.shape[0], dtype=jnp.int32)
    orbit = 2.0 * math.pi / PERIOD * (position % PERIOD).astype(jnp.float32)
    offset = 2.0 * math.pi / NGRID * phase_idx.astype(jnp.float32)
    sine = jnp.sin(offset[:, None] + orbit[None, :])
    amplitude = 8.0 + 4.0 * amplitude_idx.astype(jnp.float32)
    phase = amplitude[:, None, None] * (sine[:, partner] - sine[:, None, :span])
    rows = phase.shape[0]
    factors = jnp.concatenate([jnp.cos(phase).reshape(rows, -1).astype(jnp.bfloat16), jnp.sin(phase).reshape(rows, -1).astype(jnp.bfloat16)], 1)
    return jnp.dot(factors, stacked, preferred_element_type=jnp.float32)

def reference(sfts, detector_ids, intersection, lags, template_ids):
    power = lax.optimization_barrier(jnp.sum(sfts[:, 0] * sfts[:, 0] + sfts[:, 1] * sfts[:, 1], axis=1)) / NBIN
    white = (sfts * lax.rsqrt(power + 1e-06)[:, None, None]).astype(jnp.bfloat16)
    padded = jnp.pad(white, ((0, LAGMAX), (0, 0), (0, 0)))
    ids_padded = jnp.pad(detector_ids, (0, LAGMAX))
    total = sfts.shape[0]

    def add_block(number, totals):
        first_row = (number * SFT_DEV).astype(jnp.int32)
        extended = lax.dynamic_slice_in_dim(padded, first_row, SFT_DEV + LAGMAX, 0)
        return totals + block_term(extended, first_row, ids_padded, lags, intersection, template_ids[:, 0], template_ids[:, 1], total)
    totals = lax.fori_loop(0, total // SFT_DEV, add_block, jnp.zeros((NTEMPL, NBIN), jnp.float32))
    return totals * jnp.float32(1.0 / math.sqrt(total * NLAG))
```

```python
import functools
import math

import jax
import jax.numpy as jnp
from jax import lax
from jax.experimental import pallas as pl
from jax.experimental.pallas import tpu as pltpu
from jax.sharding import PartitionSpec as P

NBIN = 4096
LAGMAX = 16
NGRID = 64
PERIOD = 283
ROWS = 288
EROWS = ROWS + LAGMAX
LANES = 128

SIN_COEF = (4.442883014678955, -7.308245658874512, 3.606354236602783, -0.8461116552352905, 0.1098245158791542)
COS_COEF = (1.4142135381698608, -6.978850841522217, 5.739460468292236, -1.883557915687561, 0.3106880187988281)


def horner(coef, y):
    total = coef[-1] * y + coef[-2]
    for value in coef[-3::-1]:
        total = total * y + value
    return total


def sincos_turns(x):
    f = x - jnp.round(x)
    y = f * f
    s = horner(SIN_COEF, y) * f
    c = horner(COS_COEF, y)
    return s * c, 1.0 - s * s


def factor_kernel(lags_ref, ids_ref, out_ref, sa, ca, er, ei):
    lag_count = lags_ref.shape[0]

    @pl.when(pl.program_id(0) == 0)
    def _():
        def row_block(b, carry):
            r0 = pl.multiple_of(b * 8, 8)
            row = lax.broadcasted_iota(jnp.int32, (8, LANES), 0) + r0
            s, c = sincos_turns(row.astype(jnp.float32) * (1.0 / PERIOD))
            sa[pl.ds(r0, 8), :] = s
            ca[pl.ds(r0, 8), :] = c
            return carry

        lax.fori_loop(0, EROWS // 8, row_block, 0)

    ids = ids_ref[0].astype(jnp.float32)
    amplitude = (8.0 + 4.0 * ids[0:1]) * (1.0 / (2.0 * math.pi))
    sq, cq = sincos_turns(ids[1:2] * (1.0 / NGRID))
    with_sin = jnp.broadcast_to(amplitude * cq, (16, LANES))
    with_cos = jnp.broadcast_to(amplitude * sq, (16, LANES))

    def exp_block(b, carry):
        r0 = pl.multiple_of(b * 16, 16)
        s, c = sincos_turns(sa[pl.ds(r0, 16), :] * with_sin + ca[pl.ds(r0, 16), :] * with_cos)
        er[pl.ds(r0, 16), :] = c
        ei[pl.ds(r0, 16), :] = s
        return carry

    lax.fori_loop(0, EROWS // 16, exp_block, 0, unroll=True)

    def factor_block(b, carry):
        r0 = pl.multiple_of(b * 16, 16)
        cr = er[pl.ds(r0, 16), :]
        ci = ei[pl.ds(r0, 16), :]
        for l in range(lag_count):
            far = r0 + lags_ref[l]
            fr = er[pl.ds(far, 16), :]
            fi = ei[pl.ds(far, 16), :]
            at = pl.multiple_of(l * ROWS + r0, 16)
            out_ref[0, pl.ds(at, 16), :] = (fr * cr + fi * ci).astype(jnp.bfloat16)
            at = pl.multiple_of((lag_count + l) * ROWS + r0, 16)
            out_ref[0, pl.ds(at, 16), :] = (fi * cr - fr * ci).astype(jnp.bfloat16)
        return carry

    lax.fori_loop(0, ROWS // 16, factor_block, 0)


def factors(lags, ids):
    depth = 2 * lags.shape[0] * ROWS
    blocks = ids.shape[0]
    return pl.pallas_call(
        factor_kernel,
        grid=(blocks,),
        out_shape=jax.ShapeDtypeStruct((blocks // 2, depth, 2 * LANES), jnp.bfloat16),
        in_specs=[
            pl.BlockSpec(memory_space=pltpu.SMEM),
            pl.BlockSpec((1, 2, LANES), lambda i: (i, 0, 0)),
        ],
        out_specs=pl.BlockSpec((1, depth, LANES), lambda i: (i // 2, 0, i % 2)),
        scratch_shapes=[pltpu.VMEM((EROWS, LANES), jnp.float32)] * 4,
        cost_estimate=pl.CostEstimate(
            flops=blocks * LANES * depth * 30,
            bytes_accessed=blocks * LANES * depth * 2,
            transcendentals=0,
        ),
        name="factors",
    )(lags, ids)


def stat_kernel(scale, total, lags_ref, inter_ref, white_ref, det_ref, factor_hbm, out_ref, z, y, fold, factor, sems):
    lag_count = lags_ref.shape[0]
    half = lag_count * ROWS
    chunks = factor_hbm.shape[0]
    copies = [pltpu.make_async_copy(factor_hbm.at[c], factor.at[c], sems.at[c]) for c in range(chunks)]
    for copy in copies:
        copy.start()
    blocks, rows2, _ = white_ref.shape
    rows = rows2 // 2
    weights = [[inter_ref[a, b] for b in range(3)] for a in range(3)]

    def unpack(b, carry):
        at = pl.multiple_of(b * rows, 8)
        det = det_ref[pl.ds(at, rows), :]
        is0 = det == 0.0
        is1 = det == 1.0
        parts = [white_ref[b, c * rows : (c + 1) * rows, :].astype(jnp.float32) for c in range(2)]
        for c in range(2):
            z[c, pl.ds(at, rows), :] = parts[c]
        for a in range(3):
            w = jnp.where(is0, weights[a][0], jnp.where(is1, weights[a][1], weights[a][2]))
            for c in range(2):
                y[2 * a + c, pl.ds(at, rows), :] = w * parts[c]
        return carry

    lax.fori_loop(0, blocks, unpack, 0)
    rest = z.shape[1] - total
    for c in range(2):
        z[c, total:, :] = jnp.zeros((rest, LANES), jnp.float32)
    for c in range(6):
        y[c, total:, :] = jnp.zeros((rest, LANES), jnp.float32)

    def pair_block(cycles, b, carry):
        r0 = pl.multiple_of(b * 8, 8)
        lag = [lags_ref[l] for l in range(lag_count)]
        acc_re = [jnp.zeros((8, LANES), jnp.float32)] * lag_count
        acc_im = [jnp.zeros((8, LANES), jnp.float32)] * lag_count
        for m in range(cycles):
            i0 = r0 + PERIOD * m
            a = z[0, pl.ds(i0, 8), :]
            bb = z[1, pl.ds(i0, 8), :]
            det = det_ref[pl.ds(i0, 8), :]
            is0 = det == 0.0
            is1 = det == 1.0
            for l in range(lag_count):
                j0 = i0 + lag[l]
                far = []
                for c in range(2):
                    far.append(
                        jnp.where(
                            is0,
                            y[c, pl.ds(j0, 8), :],
                            jnp.where(is1, y[2 + c, pl.ds(j0, 8), :], y[4 + c, pl.ds(j0, 8), :]),
                        )
                    )
                acc_re[l] = acc_re[l] + (a * far[0] + bb * far[1])
                acc_im[l] = acc_im[l] + (a * far[1] - bb * far[0])
        for l in range(lag_count):
            fold[pl.ds(pl.multiple_of(l * ROWS + r0, 8), 8), :] = acc_re[l]
            fold[pl.ds(pl.multiple_of(half + l * ROWS + r0, 8), 8), :] = acc_im[l]
        return carry

    full = total // PERIOD
    split = -(-(total - full * PERIOD) // 8)
    lax.fori_loop(0, split, functools.partial(pair_block, full + 1), 0)
    lax.fori_loop(split, ROWS // 8, functools.partial(pair_block, full), 0)
    for l in range(2 * lag_count):
        at = l * ROWS + PERIOD
        fold[at : at + ROWS - PERIOD, :] = jnp.zeros((ROWS - PERIOD, LANES), jnp.float32)

    pairs = fold[...].astype(jnp.bfloat16)
    for c in range(chunks):
        copies[c].wait()
        sums = lax.dot_general(
            pairs, factor[c], (((0,), (0,)), ((), ())), preferred_element_type=jnp.float32
        )
        stat = (sums * scale).T.astype(jnp.bfloat16)
        out_ref[2 * c] = stat[:LANES]
        out_ref[2 * c + 1] = stat[LANES:]


def statistic(lags, intersection, white, det, factor, scale, total):
    chunks, depth, width = factor.shape
    zrows = det.shape[0]
    smem = pl.BlockSpec(memory_space=pltpu.SMEM)
    vmem = pl.BlockSpec(memory_space=pltpu.VMEM)
    return pl.pallas_call(
        functools.partial(stat_kernel, scale, total),
        out_shape=jax.ShapeDtypeStruct((2 * chunks, LANES, LANES), jnp.bfloat16),
        in_specs=[smem, smem, vmem, vmem, pl.BlockSpec(memory_space=pl.ANY)],
        out_specs=vmem,
        scratch_shapes=[
            pltpu.VMEM((2, zrows, LANES), jnp.float32),
            pltpu.VMEM((6, zrows, LANES), jnp.float32),
            pltpu.VMEM((depth, LANES), jnp.float32),
            pltpu.VMEM((chunks, depth, width), jnp.bfloat16),
            pltpu.SemaphoreType.DMA((chunks,)),
        ],
        cost_estimate=pl.CostEstimate(
            flops=2 * depth * chunks * width * LANES,
            bytes_accessed=depth * chunks * width * 2,
            transcendentals=0,
        ),
        name="statistic",
    )(lags, intersection, white, det, factor)


def shards(sfts, detector_ids, intersection, lags, template_ids):
    rows, _, bins = sfts.shape
    times = lax.axis_size("tm")
    pieces = bins // LANES
    groups = [list(range(g, g + pieces)) for g in range(0, times, pieces)]
    total = detector_ids.shape[0]
    scale = 1.0 / math.sqrt(total * lags.shape[0])

    ids = jnp.broadcast_to(template_ids.T, (pieces, 2, template_ids.shape[0]))
    ids = lax.all_to_all(ids, "tm", split_axis=0, concat_axis=0, axis_index_groups=groups, tiled=True)
    factor = factors(lags, ids)

    local_power = jnp.sum(sfts[:, 0] * sfts[:, 0] + sfts[:, 1] * sfts[:, 1], axis=1)
    power = lax.all_gather(local_power, "freq", axis=0).sum(axis=0) / NBIN
    white = (sfts * lax.rsqrt(power + 1e-06)[:, None, None]).astype(jnp.bfloat16)
    tiles = white.reshape(rows, 2, pieces, LANES).transpose(2, 1, 0, 3).reshape(pieces, 2 * rows, LANES)
    send = jnp.broadcast_to(tiles, (times // pieces, *tiles.shape)).reshape(times, 2 * rows, LANES)
    every = lax.all_to_all(send, "tm", split_axis=0, concat_axis=0, tiled=True)

    reach = PERIOD * (total // PERIOD) + ROWS + LAGMAX
    zrows = -(-reach // 16) * 16
    det = jnp.pad(detector_ids.astype(jnp.float32), (0, zrows - total))
    det = jnp.broadcast_to(det[:, None], (zrows, LANES))

    part = statistic(lags, intersection, every, det, factor, scale, total)
    mine = lax.all_to_all(part, "tm", split_axis=0, concat_axis=0, axis_index_groups=groups, tiled=True)
    return jnp.moveaxis(mine.astype(jnp.float32), 0, 1).reshape(template_ids.shape[0], bins)


def solution(mesh):
    in_specs = (P("tm", None, "freq"), P(), P(), P(), P("tm", None))
    out_specs = P("tm", "freq")
    return jax.shard_map(shards, mesh=mesh, in_specs=in_specs, out_specs=out_specs, check_vma=False)
```

```python
import functools
import math

import jax
import jax.numpy as jnp
from jax import lax
from jax.experimental import pallas as pl
from jax.experimental.pallas import tpu as pltpu
from jax.sharding import PartitionSpec as P

NBIN = 4096
LAGMAX = 16
NGRID = 64
PERIOD = 283
ROWS = 288
EROWS = ROWS + LAGMAX
LANES = 128
EXTRA = 8

SIN_COEF = (4.442883014678955, -7.308245658874512, 3.606354236602783, -0.8461116552352905, 0.1098245158791542)
COS_COEF = (1.4142135381698608, -6.978850841522217, 5.739460468292236, -1.883557915687561, 0.3106880187988281)


def horner(coef, y):
    total = coef[-1] * y + coef[-2]
    for value in coef[-3::-1]:
        total = total * y + value
    return total


def sincos_turns(x):
    f = x - jnp.round(x)
    y = f * f
    s = horner(SIN_COEF, y) * f
    c = horner(COS_COEF, y)
    return s * c, 1.0 - s * s


def send_kernel(shift_ref, sfts_ref, ids_ref, out_ref):
    rows = sfts_ref.shape[0]
    pieces = sfts_ref.shape[2] // LANES
    copies = out_ref.shape[0] // pieces
    squares = jnp.zeros((rows, LANES), jnp.float32)
    for c in range(2):
        for v in range(pieces):
            tile = sfts_ref[:, c, v * LANES : (v + 1) * LANES]
            squares = squares + tile * tile
            small = tile.astype(jnp.bfloat16)
            for u in range(copies):
                out_ref[u * pieces + v, c * rows : (c + 1) * rows, :] = small
    square = jnp.concatenate([squares, jnp.zeros((LANES - rows, LANES), jnp.float32)], 0)
    power = jnp.sum(square.T, axis=0, keepdims=True)
    power = pltpu.roll(power, shift_ref[0], 1)
    high = power.astype(jnp.bfloat16)
    rest = power - high.astype(jnp.float32)
    middle = rest.astype(jnp.bfloat16)
    low = (rest - middle.astype(jnp.float32)).astype(jnp.bfloat16)
    ids = ids_ref[...].astype(jnp.float32).astype(jnp.bfloat16)
    spare = jnp.zeros((EXTRA - 5, LANES), jnp.bfloat16)
    extra = jnp.concatenate([high, middle, low, ids, spare], 0)
    for d in range(out_ref.shape[0]):
        out_ref[d, 2 * rows :, :] = extra


def to_send(shift, sfts, ids, times):
    rows = sfts.shape[0]
    vmem = pl.BlockSpec(memory_space=pltpu.VMEM)
    return pl.pallas_call(
        send_kernel,
        out_shape=jax.ShapeDtypeStruct((times, 2 * rows + EXTRA, LANES), jnp.bfloat16),
        in_specs=[pl.BlockSpec(memory_space=pltpu.SMEM), vmem, vmem],
        out_specs=vmem,
        name="to_send",
    )(shift, sfts, ids)


def column_kernel(row_ref, out_ref):
    for b in range(row_ref.shape[0]):
        at = b * LANES
        size = min(LANES, out_ref.shape[0] - at)
        tile = jnp.broadcast_to(row_ref[b : b + 1, :], (LANES, LANES)).T
        out_ref[at : at + size, :] = tile[:size]


def columns(values, length):
    rows = -(-length // LANES)
    padded = jnp.pad(values, (0, rows * LANES - values.shape[0])).reshape(rows, LANES)
    return pl.pallas_call(
        column_kernel,
        out_shape=jax.ShapeDtypeStruct((length, LANES), jnp.float32),
        in_specs=[pl.BlockSpec(memory_space=pltpu.VMEM)],
        out_specs=pl.BlockSpec(memory_space=pltpu.VMEM),
        cost_estimate=pl.CostEstimate(flops=length * LANES * 1000, bytes_accessed=length * LANES * 4, transcendentals=0),
        name="columns",
    )(padded)


def factor_kernel(lags_ref, first_ref, every_ref, out_ref, sa, ca, er, ei):
    lag_count = lags_ref.shape[0]
    step = pl.program_id(0)

    @pl.when(step == 0)
    def _():
        for b in range(EROWS // 16):
            r0 = b * 16
            row = lax.broadcasted_iota(jnp.int32, (16, LANES), 0) + r0
            s, c = sincos_turns(row.astype(jnp.float32) * (1.0 / PERIOD))
            sa[pl.ds(r0, 16), :] = s
            ca[pl.ds(r0, 16), :] = c

    ids = every_ref[first_ref[0] + step].astype(jnp.float32)
    amplitude = (8.0 + 4.0 * ids[3:4]) * (1.0 / (2.0 * math.pi))
    sq, cq = sincos_turns(ids[4:5] * (1.0 / NGRID))
    with_sin = jnp.broadcast_to(amplitude * cq, (16, LANES))
    with_cos = jnp.broadcast_to(amplitude * sq, (16, LANES))
    for b in range(EROWS // 16):
        r0 = b * 16
        s, c = sincos_turns(sa[pl.ds(r0, 16), :] * with_sin + ca[pl.ds(r0, 16), :] * with_cos)
        er[pl.ds(r0, 16), :] = c
        ei[pl.ds(r0, 16), :] = s

    def lag_block(l, carry):
        lag = lags_ref[l]
        at = l * (ROWS // 16)
        half = lag_count * (ROWS // 16)
        for b in range(ROWS // 16):
            r0 = b * 16
            cr = er[pl.ds(r0, 16), :]
            ci = ei[pl.ds(r0, 16), :]
            fr = er[pl.ds(lag + r0, 16), :]
            fi = ei[pl.ds(lag + r0, 16), :]
            out_ref[0, at + b] = (fr * cr + fi * ci).astype(jnp.bfloat16)
            out_ref[0, at + (half + b)] = (fi * cr - fr * ci).astype(jnp.bfloat16)
        return carry

    lax.fori_loop(0, lag_count, lag_block, 0)


def factors(lags, first, every, blocks, across):
    depth = 2 * lags.shape[0] * ROWS
    devices, rows, _ = every.shape
    smem = pl.BlockSpec(memory_space=pltpu.SMEM)
    return pl.pallas_call(
        factor_kernel,
        grid=(blocks,),
        out_shape=jax.ShapeDtypeStruct((blocks // across, depth // 16, 16, across * LANES), jnp.bfloat16),
        in_specs=[smem, smem, pl.BlockSpec((devices, EXTRA, LANES), lambda i: (0, rows // EXTRA - 1, 0))],
        out_specs=pl.BlockSpec((1, depth // 16, 16, LANES), lambda i: (i // across, 0, 0, i % across)),
        scratch_shapes=[pltpu.VMEM((EROWS, LANES), jnp.float32)] * 4,
        cost_estimate=pl.CostEstimate(
            flops=blocks * LANES * depth * 30,
            bytes_accessed=blocks * LANES * depth * 2,
            transcendentals=0,
        ),
        name="factors",
    )(lags, first, every)


def stat_kernel(
    scale, total, lags_ref, inter_ref, every_ref, det_ref, power_ref, factor_hbm, out_ref, z, y, fold, pairs, factor, sems
):
    lag_count = lags_ref.shape[0]
    half = lag_count * ROWS
    chunks, depth, width = factor_hbm.shape
    copies = [pltpu.make_async_copy(factor_hbm.at[c], factor.at[c], sems.at[c]) for c in range(chunks)]
    for copy in copies:
        copy.start()
    devices, rows, _ = every_ref.shape
    rows = (rows - EXTRA) // 2
    weights = [[inter_ref[a, b] for b in range(3)] for a in range(3)]

    powers = power_ref[0]
    for q in range(1, power_ref.shape[0]):
        powers = powers + power_ref[q]
    factor_of = lax.rsqrt(powers * (1.0 / NBIN) + 1e-06)
    lane = lax.broadcasted_iota(jnp.int32, (1, LANES), 1)
    for g in range(total // LANES):
        first = g * LANES // rows
        last = (g * LANES + LANES - 1) // rows
        line = factor_of[first : first + 1]
        for d in range(first + 1, last + 1):
            line = jnp.where(lane < d * rows - g * LANES, line, factor_of[d : d + 1])
        column = jnp.broadcast_to(line, (LANES, LANES)).T
        for h in range(LANES // 16):
            i0 = g * LANES + h * 16
            d, r = divmod(i0, rows)
            det = det_ref[i0 : i0 + 16, :]
            is0 = det == 0.0
            is1 = det == 1.0
            parts = []
            for c in range(2):
                raw = every_ref[d, c * rows + r : c * rows + r + 16, :].astype(jnp.float32)
                part = raw * column[h * 16 : h * 16 + 16]
                parts.append(part)
                z[c, i0 : i0 + 16, :] = part
            for a in range(3):
                w = jnp.where(is0, weights[a][0], jnp.where(is1, weights[a][1], weights[a][2]))
                for c in range(2):
                    y[2 * a + c, i0 : i0 + 16, :] = w * parts[c]
    rest = z.shape[1] - total
    for c in range(2):
        z[c, total:, :] = jnp.zeros((rest, LANES), jnp.float32)
    for c in range(6):
        y[c, total:, :] = jnp.zeros((rest, LANES), jnp.float32)

    def pair_block(cycles, b, carry):
        r0 = pl.multiple_of(b * 8, 8)
        lag = [lags_ref[l] for l in range(lag_count)]
        acc_re = [None] * lag_count
        acc_im = [None] * lag_count
        for m in range(cycles):
            i0 = r0 + PERIOD * m
            a = z[0, pl.ds(i0, 8), :]
            bb = z[1, pl.ds(i0, 8), :]
            det = det_ref[pl.ds(i0, 8), :]
            is0 = det == 0.0
            is1 = det == 1.0
            for l in range(lag_count):
                j0 = i0 + lag[l]
                far = []
                for c in range(2):
                    far.append(
                        jnp.where(
                            is0,
                            y[c, pl.ds(j0, 8), :],
                            jnp.where(is1, y[2 + c, pl.ds(j0, 8), :], y[4 + c, pl.ds(j0, 8), :]),
                        )
                    )
                re = a * far[0] + bb * far[1]
                im = a * far[1] - bb * far[0]
                acc_re[l] = re if m == 0 else acc_re[l] + re
                acc_im[l] = im if m == 0 else acc_im[l] + im
        for l in range(lag_count):
            fold[pl.ds(pl.multiple_of(l * ROWS + r0, 8), 8), :] = acc_re[l]
            fold[pl.ds(pl.multiple_of(half + l * ROWS + r0, 8), 8), :] = acc_im[l]
        return carry

    full = total // PERIOD
    split = -(-(total - full * PERIOD) // 8)
    lax.fori_loop(0, split, functools.partial(pair_block, full + 1), 0)
    lax.fori_loop(split, ROWS // 8, functools.partial(pair_block, full), 0)
    for l in range(2 * lag_count):
        at = l * ROWS + PERIOD
        fold[at : at + ROWS - PERIOD, :] = jnp.zeros((ROWS - PERIOD, LANES), jnp.float32)

    for b in range(depth // LANES):
        pairs[:, b * LANES : (b + 1) * LANES] = fold[b * LANES : (b + 1) * LANES, :].T.astype(jnp.bfloat16)

    for c in range(chunks):
        copies[c].wait()
        sums = jnp.dot(pairs[...], factor[c], preferred_element_type=jnp.float32) * scale
        for h in range(width // LANES):
            out_ref[c * (width // LANES) + h] = sums[:, h * LANES : (h + 1) * LANES].T.astype(jnp.bfloat16)


def statistic(lags, intersection, every, det, power, factor, scale, total):
    chunks, depth, width = factor.shape
    zrows = det.shape[0]
    smem = pl.BlockSpec(memory_space=pltpu.SMEM)
    vmem = pl.BlockSpec(memory_space=pltpu.VMEM)
    return pl.pallas_call(
        functools.partial(stat_kernel, scale, total),
        out_shape=jax.ShapeDtypeStruct((chunks * width // LANES, LANES, LANES), jnp.bfloat16),
        in_specs=[smem, smem, vmem, vmem, vmem, pl.BlockSpec(memory_space=pl.ANY)],
        out_specs=vmem,
        scratch_shapes=[
            pltpu.VMEM((2, zrows, LANES), jnp.float32),
            pltpu.VMEM((6, zrows, LANES), jnp.float32),
            pltpu.VMEM((depth, LANES), jnp.float32),
            pltpu.VMEM((LANES, depth), jnp.bfloat16),
            pltpu.VMEM((chunks, depth, width), jnp.bfloat16),
            pltpu.SemaphoreType.DMA((chunks,)),
        ],
        cost_estimate=pl.CostEstimate(
            flops=2 * depth * chunks * width * LANES,
            bytes_accessed=depth * chunks * width * 2,
            transcendentals=0,
        ),
        name="statistic",
    )(lags, intersection, every, det, power, factor)


def shards(sfts, detector_ids, intersection, lags, template_ids):
    rows, _, bins = sfts.shape
    times = lax.axis_size("tm")
    quarters = lax.axis_size("freq")
    pieces = bins // LANES
    groups = [list(range(g, g + pieces)) for g in range(0, times, pieces)]
    total = detector_ids.shape[0]
    scale = 1.0 / math.sqrt(total * lags.shape[0])
    place = lax.axis_index("tm").astype(jnp.int32)

    send = to_send((place * rows % LANES)[None], sfts, template_ids.T, times)
    every = lax.all_to_all(send, "tm", split_axis=0, concat_axis=0, tiled=True)

    power = every[:, 2 * rows : 2 * rows + 3].astype(jnp.float32).sum(axis=1)
    power = jnp.broadcast_to(power, (quarters, *power.shape))
    power = lax.all_to_all(power, "freq", split_axis=0, concat_axis=0, tiled=True)

    reach = PERIOD * (total // PERIOD) + ROWS + LAGMAX
    det = columns(detector_ids.astype(jnp.float32), -(-reach // 16) * 16)

    factor = factors(lags, (place // pieces * pieces)[None], every, pieces, 4)
    factor = factor.reshape(factor.shape[0], -1, factor.shape[3])
    part = statistic(lags, intersection, every, det, power, factor, scale, total)
    mine = lax.all_to_all(part, "tm", split_axis=0, concat_axis=0, axis_index_groups=groups, tiled=True)
    return jnp.moveaxis(mine.astype(jnp.float32), 0, 1).reshape(template_ids.shape[0], bins)


def solution(mesh):
    in_specs = (P("tm", None, "freq"), P(), P(), P(), P("tm", None))
    out_specs = P("tm", "freq")
    return jax.shard_map(shards, mesh=mesh, in_specs=in_specs, out_specs=out_specs, check_vma=False)
```

```python
import functools
import math

import jax
import jax.numpy as jnp
from jax import lax
from jax.experimental import pallas as pl
from jax.experimental.pallas import tpu as pltpu
from jax.sharding import PartitionSpec as P

NBIN = 4096
LAGMAX = 16
NGRID = 64
PERIOD = 283
ROWS = 288
EROWS = ROWS + LAGMAX
LANES = 128
EXTRA = 8

SIN_COEF = (4.442883014678955, -7.308245658874512, 3.606354236602783, -0.8461116552352905, 0.1098245158791542)
COS_COEF = (1.4142135381698608, -6.978850841522217, 5.739460468292236, -1.883557915687561, 0.3106880187988281)


def horner(coef, y):
    total = coef[-1] * y + coef[-2]
    for value in coef[-3::-1]:
        total = total * y + value
    return total


def sincos_turns(x):
    f = x - jnp.round(x)
    y = f * f
    s = horner(SIN_COEF, y) * f
    c = horner(COS_COEF, y)
    return s * c, 1.0 - s * s


def send_kernel(shift_ref, sfts_ref, ids_ref, out_ref):
    rows = sfts_ref.shape[0]
    pieces = sfts_ref.shape[2] // LANES
    copies = out_ref.shape[0] // pieces
    squares = jnp.zeros((rows, LANES), jnp.float32)
    for c in range(2):
        for v in range(pieces):
            tile = sfts_ref[:, c, v * LANES : (v + 1) * LANES]
            squares = squares + tile * tile
            small = tile.astype(jnp.bfloat16)
            for u in range(copies):
                out_ref[u * pieces + v, c * rows : (c + 1) * rows, :] = small
    square = jnp.concatenate([squares, jnp.zeros((LANES - rows, LANES), jnp.float32)], 0)
    power = jnp.sum(square.T, axis=0, keepdims=True)
    power = pltpu.roll(power, shift_ref[0], 1)
    high = power.astype(jnp.bfloat16)
    rest = power - high.astype(jnp.float32)
    middle = rest.astype(jnp.bfloat16)
    low = (rest - middle.astype(jnp.float32)).astype(jnp.bfloat16)
    ids = ids_ref[...].astype(jnp.float32).astype(jnp.bfloat16)
    spare = jnp.zeros((EXTRA - 5, LANES), jnp.bfloat16)
    extra = jnp.concatenate([high, middle, low, ids, spare], 0)
    for d in range(out_ref.shape[0]):
        out_ref[d, 2 * rows :, :] = extra


def to_send(shift, sfts, ids, times):
    rows = sfts.shape[0]
    vmem = pl.BlockSpec(memory_space=pltpu.VMEM)
    return pl.pallas_call(
        send_kernel,
        out_shape=jax.ShapeDtypeStruct((times, 2 * rows + EXTRA, LANES), jnp.bfloat16),
        in_specs=[pl.BlockSpec(memory_space=pltpu.SMEM), vmem, vmem],
        out_specs=vmem,
        name="to_send",
    )(shift, sfts, ids)


def stat_kernel(
    scale,
    total,
    lags_ref,
    inter_ref,
    first_ref,
    every_ref,
    det_row_ref,
    power_ref,
    out_ref,
    z,
    y,
    det,
    fold,
    pairs,
    sa,
    ca,
    er,
    ei,
    nr,
    ni,
):
    lag_count = lags_ref.shape[0]
    devices, rows, _ = every_ref.shape
    rows = (rows - EXTRA) // 2
    blocks = out_ref.shape[0]
    weights = [[inter_ref[a, b] for b in range(3)] for a in range(3)]

    powers = power_ref[0]
    for q in range(1, power_ref.shape[0]):
        powers = powers + power_ref[q]
    factor_of = lax.rsqrt(powers * (1.0 / NBIN) + 1e-06)
    lane = lax.broadcasted_iota(jnp.int32, (1, LANES), 1)
    for g in range(total // LANES):
        first = g * LANES // rows
        last = (g * LANES + LANES - 1) // rows
        line = factor_of[first : first + 1]
        for d in range(first + 1, last + 1):
            line = jnp.where(lane < d * rows - g * LANES, line, factor_of[d : d + 1])
        column = jnp.broadcast_to(line, (LANES, LANES)).T
        dets = jnp.broadcast_to(det_row_ref[g : g + 1, :].astype(jnp.float32), (LANES, LANES)).T
        det[g * LANES : (g + 1) * LANES, :] = dets
        for h in range(LANES // 16):
            i0 = g * LANES + h * 16
            d, r = divmod(i0, rows)
            here = dets[h * 16 : h * 16 + 16]
            is0 = here == 0.0
            is1 = here == 1.0
            parts = []
            for c in range(2):
                raw = every_ref[d, c * rows + r : c * rows + r + 16, :].astype(jnp.float32)
                part = raw * column[h * 16 : h * 16 + 16]
                parts.append(part)
                z[c, i0 : i0 + 16, :] = part
            for a in range(3):
                w = jnp.where(is0, weights[a][0], jnp.where(is1, weights[a][1], weights[a][2]))
                for c in range(2):
                    y[2 * a + c, i0 : i0 + 16, :] = w * parts[c]
    rest = z.shape[1] - total
    det[total:, :] = jnp.zeros((rest, LANES), jnp.float32)
    for c in range(2):
        z[c, total:, :] = jnp.zeros((rest, LANES), jnp.float32)
    for c in range(6):
        y[c, total:, :] = jnp.zeros((rest, LANES), jnp.float32)

    for b in range(EROWS // 16):
        r0 = b * 16
        row = lax.broadcasted_iota(jnp.int32, (16, LANES), 0) + r0
        s, c = sincos_turns(row.astype(jnp.float32) * (1.0 / PERIOD))
        sa[r0 : r0 + 16, :] = s
        ca[r0 : r0 + 16, :] = c

    def exp_block(t, carry):
        ids = every_ref[first_ref[0] + t, 2 * rows : 2 * rows + EXTRA, :].astype(jnp.float32)
        amplitude = (8.0 + 4.0 * ids[3:4]) * (1.0 / (2.0 * math.pi))
        sq, cq = sincos_turns(ids[4:5] * (1.0 / NGRID))
        with_sin = jnp.broadcast_to(amplitude * cq, (16, LANES))
        with_cos = jnp.broadcast_to(amplitude * sq, (16, LANES))
        for b in range(EROWS // 16):
            r0 = b * 16
            s, c = sincos_turns(sa[r0 : r0 + 16, :] * with_sin + ca[r0 : r0 + 16, :] * with_cos)
            er[t, r0 : r0 + 16, :] = c
            ei[t, r0 : r0 + 16, :] = s
            if r0 < ROWS:
                nr[t, r0 : r0 + 16, :] = c.astype(jnp.bfloat16)
                ni[t, r0 : r0 + 16, :] = s.astype(jnp.bfloat16)
        return carry

    lax.fori_loop(0, blocks, exp_block, 0)

    def pair_block(cycles, b, carry):
        r0 = pl.multiple_of(b * 8, 8)
        lag = [lags_ref[l] for l in range(lag_count)]
        acc_re = [None] * lag_count
        acc_im = [None] * lag_count
        for m in range(cycles):
            i0 = r0 + PERIOD * m
            a = z[0, pl.ds(i0, 8), :]
            bb = z[1, pl.ds(i0, 8), :]
            here = det[pl.ds(i0, 8), :]
            is0 = here == 0.0
            is1 = here == 1.0
            for l in range(lag_count):
                j0 = i0 + lag[l]
                far = []
                for c in range(2):
                    far.append(
                        jnp.where(
                            is0,
                            y[c, pl.ds(j0, 8), :],
                            jnp.where(is1, y[2 + c, pl.ds(j0, 8), :], y[4 + c, pl.ds(j0, 8), :]),
                        )
                    )
                re = a * far[0] + bb * far[1]
                im = a * far[1] - bb * far[0]
                acc_re[l] = re if m == 0 else acc_re[l] + re
                acc_im[l] = im if m == 0 else acc_im[l] + im
        for l in range(lag_count):
            fold[pl.ds(pl.multiple_of(2 * l * ROWS + r0, 8), 8), :] = acc_re[l]
            fold[pl.ds(pl.multiple_of((2 * l + 1) * ROWS + r0, 8), 8), :] = acc_im[l]
        return carry

    full = total // PERIOD
    split = -(-(total - full * PERIOD) // 8)
    lax.fori_loop(0, split, functools.partial(pair_block, full + 1), 0)
    lax.fori_loop(split, ROWS // 8, functools.partial(pair_block, full), 0)
    for l in range(2 * lag_count):
        at = l * ROWS + PERIOD
        fold[at : at + ROWS - PERIOD, :] = jnp.zeros((ROWS - PERIOD, LANES), jnp.float32)

    wide = 4
    step = 2 * 2 * ROWS
    sums = [None] * (blocks // wide)
    for k in range(lag_count // 2):
        for b in range(step // LANES):
            at = k * step + b * LANES
            pairs[:, at : at + LANES] = fold[at : at + LANES, :].T.astype(jnp.bfloat16)
        for n in range(blocks // wide):
            columns = []
            for t in range(n * wide, (n + 1) * wide):
                column = []
                for l in (2 * k, 2 * k + 1):
                    lag = lags_ref[l]
                    cos_rows = []
                    sin_rows = []
                    for b in range(ROWS // 16):
                        r0 = b * 16
                        cr = nr[t, r0 : r0 + 16, :]
                        ci = ni[t, r0 : r0 + 16, :]
                        fr = er[t, pl.ds(lag + r0, 16), :].astype(jnp.bfloat16)
                        fi = ei[t, pl.ds(lag + r0, 16), :].astype(jnp.bfloat16)
                        cos_rows.append(fr * cr + fi * ci)
                        sin_rows.append(fi * cr - fr * ci)
                    column += cos_rows + sin_rows
                columns.append(jnp.concatenate(column, 0))
            term = jnp.dot(
                pairs[:, k * step : (k + 1) * step],
                jnp.concatenate(columns, 1),
                preferred_element_type=jnp.float32,
            )
            sums[n] = term if k == 0 else sums[n] + term
    for n in range(blocks // wide):
        for h in range(wide):
            out_ref[n * wide + h] = (sums[n][:, h * LANES : (h + 1) * LANES] * scale).T.astype(jnp.bfloat16)


def statistic(lags, intersection, first, every, det, power, blocks, scale):
    total = det.size
    depth = 2 * lags.shape[0] * ROWS
    reach = PERIOD * (total // PERIOD) + ROWS + LAGMAX
    zrows = -(-reach // 16) * 16
    smem = pl.BlockSpec(memory_space=pltpu.SMEM)
    vmem = pl.BlockSpec(memory_space=pltpu.VMEM)
    f32 = jnp.float32
    return pl.pallas_call(
        functools.partial(stat_kernel, scale, total),
        out_shape=jax.ShapeDtypeStruct((blocks, LANES, LANES), jnp.bfloat16),
        in_specs=[smem, smem, smem, vmem, vmem, vmem],
        out_specs=vmem,
        scratch_shapes=[
            pltpu.VMEM((2, zrows, LANES), f32),
            pltpu.VMEM((6, zrows, LANES), f32),
            pltpu.VMEM((zrows, LANES), f32),
            pltpu.VMEM((depth, LANES), f32),
            pltpu.VMEM((LANES, depth), jnp.bfloat16),
            pltpu.VMEM((EROWS, LANES), f32),
            pltpu.VMEM((EROWS, LANES), f32),
            pltpu.VMEM((blocks, EROWS, LANES), f32),
            pltpu.VMEM((blocks, EROWS, LANES), f32),
            pltpu.VMEM((blocks, ROWS, LANES), jnp.bfloat16),
            pltpu.VMEM((blocks, ROWS, LANES), jnp.bfloat16),
        ],
        cost_estimate=pl.CostEstimate(
            flops=2 * depth * blocks * LANES * LANES, bytes_accessed=every.size * 2, transcendentals=0
        ),
        name="statistic",
    )(lags, intersection, first, every, det, power)


def shards(sfts, detector_ids, intersection, lags, template_ids):
    rows, _, bins = sfts.shape
    times = lax.axis_size("tm")
    quarters = lax.axis_size("freq")
    pieces = bins // LANES
    groups = [list(range(g, g + pieces)) for g in range(0, times, pieces)]
    total = detector_ids.shape[0]
    scale = 1.0 / math.sqrt(total * lags.shape[0])
    place = lax.axis_index("tm").astype(jnp.int32)

    send = to_send((place * rows % LANES)[None], sfts, template_ids.T, times)
    every = lax.all_to_all(send, "tm", split_axis=0, concat_axis=0, tiled=True)
    every, detector_ids, place = lax.optimization_barrier((every, detector_ids, place))

    power = every[:, 2 * rows : 2 * rows + 3].astype(jnp.float32).sum(axis=1)
    power = lax.all_gather(power, "freq", axis=0, tiled=True).reshape(quarters, *power.shape)
    power, detector_ids = lax.optimization_barrier((power, detector_ids))

    det = detector_ids.reshape(total // LANES, LANES)
    part = statistic(lags, intersection, (place // pieces * pieces)[None], every, det, power, pieces, scale)
    mine = lax.all_to_all(part, "tm", split_axis=0, concat_axis=0, axis_index_groups=groups, tiled=True)
    return jnp.moveaxis(mine.astype(jnp.float32), 0, 1).reshape(template_ids.shape[0], bins)


def solution(mesh):
    in_specs = (P("tm", None, "freq"), P(), P(), P(), P("tm", None))
    out_specs = P("tm", "freq")
    return jax.shard_map(shards, mesh=mesh, in_specs=in_specs, out_specs=out_specs, check_vma=False)
```

```python
import functools
import math

import jax
import jax.numpy as jnp
from jax import lax
from jax.experimental import pallas as pl
from jax.experimental.pallas import tpu as pltpu
from jax.sharding import PartitionSpec as P

NBIN = 4096
LAGMAX = 16
NGRID = 64
PERIOD = 283
ROWS = 288
EROWS = ROWS + LAGMAX
LANES = 128
EXTRA = 8

SIN_COEF = (4.442883014678955, -7.308245658874512, 3.606354236602783, -0.8461116552352905, 0.1098245158791542)
COS_COEF = (1.4142135381698608, -6.978850841522217, 5.739460468292236, -1.883557915687561, 0.3106880187988281)


def horner(coef, y):
    total = coef[-1] * y + coef[-2]
    for value in coef[-3::-1]:
        total = total * y + value
    return total


def sincos_turns(x):
    f = x - jnp.round(x)
    y = f * f
    s = horner(SIN_COEF, y) * f
    c = horner(COS_COEF, y)
    return s * c, 1.0 - s * s


def send_kernel(shift_ref, sfts_ref, ids_ref, out_ref):
    rows = sfts_ref.shape[0]
    pieces = sfts_ref.shape[2] // LANES
    copies = out_ref.shape[0] // pieces
    squares = jnp.zeros((rows, LANES), jnp.float32)
    for c in range(2):
        for v in range(pieces):
            tile = sfts_ref[:, c, v * LANES : (v + 1) * LANES]
            squares = squares + tile * tile
            small = tile.astype(jnp.bfloat16)
            for u in range(copies):
                out_ref[u * pieces + v, c * rows : (c + 1) * rows, :] = small
    square = jnp.concatenate([squares, jnp.zeros((LANES - rows, LANES), jnp.float32)], 0)
    power = jnp.sum(square.T, axis=0, keepdims=True)
    power = pltpu.roll(power, shift_ref[0], 1)
    high = power.astype(jnp.bfloat16)
    rest = power - high.astype(jnp.float32)
    middle = rest.astype(jnp.bfloat16)
    low = (rest - middle.astype(jnp.float32)).astype(jnp.bfloat16)
    ids = ids_ref[...].astype(jnp.float32).astype(jnp.bfloat16)
    spare = jnp.zeros((EXTRA - 5, LANES), jnp.bfloat16)
    extra = jnp.concatenate([high, middle, low, ids, spare], 0)
    for d in range(out_ref.shape[0]):
        out_ref[d, 2 * rows :, :] = extra


def to_send(shift, sfts, ids, times):
    rows = sfts.shape[0]
    vmem = pl.BlockSpec(memory_space=pltpu.VMEM)
    return pl.pallas_call(
        send_kernel,
        out_shape=jax.ShapeDtypeStruct((times, 2 * rows + EXTRA, LANES), jnp.bfloat16),
        in_specs=[pl.BlockSpec(memory_space=pltpu.SMEM), vmem, vmem],
        out_specs=vmem,
        name="to_send",
    )(shift, sfts, ids)


def stat_kernel(
    scale,
    total,
    lags_ref,
    inter_ref,
    first_ref,
    every_ref,
    det_row_ref,
    power_ref,
    out_ref,
    z,
    y,
    det,
    fold,
    pairs,
    sa,
    ca,
    far,
    near,
):
    lag_count = lags_ref.shape[0]
    devices, rows, _ = every_ref.shape
    rows = (rows - EXTRA) // 2
    blocks = out_ref.shape[0]
    weights = [[inter_ref[a, b] for b in range(3)] for a in range(3)]

    powers = power_ref[0]
    for q in range(1, power_ref.shape[0]):
        powers = powers + power_ref[q]
    factor_of = lax.rsqrt(powers * (1.0 / NBIN) + 1e-06)
    lane = lax.broadcasted_iota(jnp.int32, (1, LANES), 1)
    for g in range(total // LANES):
        first = g * LANES // rows
        last = (g * LANES + LANES - 1) // rows
        line = factor_of[first : first + 1]
        for d in range(first + 1, last + 1):
            line = jnp.where(lane < d * rows - g * LANES, line, factor_of[d : d + 1])
        column = jnp.broadcast_to(line, (LANES, LANES)).T
        dets = jnp.broadcast_to(det_row_ref[g : g + 1, :].astype(jnp.float32), (LANES, LANES)).T
        det[g * LANES : (g + 1) * LANES, :] = dets
        for h in range(LANES // 16):
            i0 = g * LANES + h * 16
            d, r = divmod(i0, rows)
            here = dets[h * 16 : h * 16 + 16]
            is0 = here == 0.0
            is1 = here == 1.0
            parts = []
            for c in range(2):
                raw = every_ref[d, c * rows + r : c * rows + r + 16, :].astype(jnp.float32)
                part = raw * column[h * 16 : h * 16 + 16]
                parts.append(part)
                z[c, i0 : i0 + 16, :] = part
            for a in range(3):
                w = jnp.where(is0, weights[a][0], jnp.where(is1, weights[a][1], weights[a][2]))
                for c in range(2):
                    y[3 * c + a, i0 : i0 + 16, :] = w * parts[c]
    rest = z.shape[1] - total
    det[total:, :] = jnp.zeros((rest, LANES), jnp.float32)
    for c in range(2):
        z[c, total:, :] = jnp.zeros((rest, LANES), jnp.float32)
    for c in range(6):
        y[c, total:, :] = jnp.zeros((rest, LANES), jnp.float32)

    for b in range(EROWS // 16):
        r0 = b * 16
        row = lax.broadcasted_iota(jnp.int32, (16, LANES), 0) + r0
        s, c = sincos_turns(row.astype(jnp.float32) * (1.0 / PERIOD))
        sa[r0 : r0 + 16, :] = s
        ca[r0 : r0 + 16, :] = c

    def exp_block(t, carry):
        ids = every_ref[first_ref[0] + t, 2 * rows : 2 * rows + EXTRA, :].astype(jnp.float32)
        amplitude = (8.0 + 4.0 * ids[3:4]) * (1.0 / (2.0 * math.pi))
        sq, cq = sincos_turns(ids[4:5] * (1.0 / NGRID))
        with_sin = jnp.broadcast_to(amplitude * cq, (16, LANES))
        with_cos = jnp.broadcast_to(amplitude * sq, (16, LANES))
        for b in range(EROWS // 16):
            r0 = b * 16
            s, c = sincos_turns(sa[r0 : r0 + 16, :] * with_sin + ca[r0 : r0 + 16, :] * with_cos)
            far[t, 0, r0 : r0 + 16, :] = c
            far[t, 1, r0 : r0 + 16, :] = s
            if r0 < ROWS:
                near[t, 0, r0 : r0 + 16, :] = c.astype(jnp.bfloat16)
                near[t, 1, r0 : r0 + 16, :] = s.astype(jnp.bfloat16)
        return carry

    lax.fori_loop(0, blocks, exp_block, 0)

    def pair_block(cycles, b, carry):
        r0 = pl.multiple_of(b * 8, 8)
        lag = [lags_ref[l] for l in range(lag_count)]
        acc_re = [None] * lag_count
        acc_im = [None] * lag_count
        for m in range(cycles):
            i0 = r0 + PERIOD * m
            a = z[0, pl.ds(i0, 8), :]
            bb = z[1, pl.ds(i0, 8), :]
            here = det[pl.ds(i0, 8), :]
            is0 = here == 0.0
            is1 = here == 1.0
            for l in range(lag_count):
                j0 = i0 + lag[l]
                other = []
                for c in range(2):
                    other.append(
                        jnp.where(
                            is0,
                            y[3 * c, pl.ds(j0, 8), :],
                            jnp.where(is1, y[3 * c + 1, pl.ds(j0, 8), :], y[3 * c + 2, pl.ds(j0, 8), :]),
                        )
                    )
                re = a * other[0] + bb * other[1]
                im = a * other[1] - bb * other[0]
                acc_re[l] = re if m == 0 else acc_re[l] + re
                acc_im[l] = im if m == 0 else acc_im[l] + im
        at = pl.multiple_of(b // 2 * 32 + b % 2 * 8, 8)
        for l in range(lag_count):
            fold[pl.ds(pl.multiple_of(2 * l * ROWS + at, 8), 8), :] = acc_re[l]
            fold[pl.ds(pl.multiple_of(2 * l * ROWS + 16 + at, 8), 8), :] = acc_im[l]
        return carry

    full = total // PERIOD
    split = -(-(total - full * PERIOD) // 8)
    lax.fori_loop(0, split, functools.partial(pair_block, full + 1), 0)
    lax.fori_loop(split, ROWS // 8, functools.partial(pair_block, full), 0)
    for l in range(lag_count):
        for c in range(2):
            at = 2 * (l + 1) * ROWS - 16 * (1 - c) - (ROWS - PERIOD)
            fold[at : at + ROWS - PERIOD, :] = jnp.zeros((ROWS - PERIOD, LANES), jnp.float32)

    wide = 4
    deep = 256
    spans = ROWS // 16
    lag = [lags_ref[l] for l in range(lag_count)]
    sums = [None] * (blocks // wide)
    for k in range(2 * lag_count * ROWS // deep):
        for b in range(deep // LANES):
            at = k * deep + b * LANES
            pairs[:, at : at + LANES] = fold[at : at + LANES, :].T.astype(jnp.bfloat16)
        for n in range(blocks // wide):
            columns = []
            for t in range(n * wide, (n + 1) * wide):
                column = []
                for q in range(k * deep // 32, (k + 1) * deep // 32):
                    l, b = divmod(q, spans)
                    r0 = b * 16
                    cr = near[t, 0, r0 : r0 + 16, :]
                    ci = near[t, 1, r0 : r0 + 16, :]
                    fr = far[t, 0, pl.ds(lag[l] + r0, 16), :].astype(jnp.bfloat16)
                    fi = far[t, 1, pl.ds(lag[l] + r0, 16), :].astype(jnp.bfloat16)
                    column += [fr * cr + fi * ci, fi * cr - fr * ci]
                columns.append(jnp.concatenate(column, 0))
            term = jnp.dot(
                pairs[:, k * deep : (k + 1) * deep],
                jnp.concatenate(columns, 1),
                preferred_element_type=jnp.float32,
            )
            sums[n] = term if k == 0 else sums[n] + term
    for n in range(blocks // wide):
        for h in range(wide):
            out_ref[n * wide + h] = (sums[n][:, h * LANES : (h + 1) * LANES] * scale).T.astype(jnp.bfloat16)


def statistic(lags, intersection, first, every, det, power, blocks, scale):
    total = det.size
    depth = 2 * lags.shape[0] * ROWS
    reach = PERIOD * (total // PERIOD) + ROWS + LAGMAX
    zrows = -(-reach // 32) * 32 + 8
    smem = pl.BlockSpec(memory_space=pltpu.SMEM)
    vmem = pl.BlockSpec(memory_space=pltpu.VMEM)
    f32 = jnp.float32
    return pl.pallas_call(
        functools.partial(stat_kernel, scale, total),
        out_shape=jax.ShapeDtypeStruct((blocks, LANES, LANES), jnp.bfloat16),
        in_specs=[smem, smem, smem, vmem, vmem, vmem],
        out_specs=vmem,
        scratch_shapes=[
            pltpu.VMEM((2, zrows, LANES), f32),
            pltpu.VMEM((6, zrows, LANES), f32),
            pltpu.VMEM((zrows, LANES), f32),
            pltpu.VMEM((depth, LANES), f32),
            pltpu.VMEM((LANES, depth), jnp.bfloat16),
            pltpu.VMEM((EROWS, LANES), f32),
            pltpu.VMEM((EROWS, LANES), f32),
            pltpu.VMEM((blocks, 2, EROWS, LANES), f32),
            pltpu.VMEM((blocks, 2, ROWS, LANES), jnp.bfloat16),
        ],
        cost_estimate=pl.CostEstimate(
            flops=2 * depth * blocks * LANES * LANES, bytes_accessed=every.size * 2, transcendentals=0
        ),
        name="statistic",
    )(lags, intersection, first, every, det, power)


def shards(sfts, detector_ids, intersection, lags, template_ids):
    rows, _, bins = sfts.shape
    times = lax.axis_size("tm")
    quarters = lax.axis_size("freq")
    pieces = bins // LANES
    groups = [list(range(g, g + pieces)) for g in range(0, times, pieces)]
    total = detector_ids.shape[0]
    scale = 1.0 / math.sqrt(total * lags.shape[0])
    place = lax.axis_index("tm").astype(jnp.int32)

    send = to_send((place * rows % LANES)[None], sfts, template_ids.T, times)
    every = lax.all_to_all(send, "tm", split_axis=0, concat_axis=0, tiled=True)
    every, detector_ids, place = lax.optimization_barrier((every, detector_ids, place))

    power = every[:, 2 * rows : 2 * rows + 3].astype(jnp.float32).sum(axis=1)
    power = lax.all_gather(power, "freq", axis=0, tiled=True).reshape(quarters, *power.shape)
    power, detector_ids = lax.optimization_barrier((power, detector_ids))

    det = detector_ids.reshape(total // LANES, LANES)
    part = statistic(lags, intersection, (place // pieces * pieces)[None], every, det, power, pieces, scale)
    mine = lax.all_to_all(part, "tm", split_axis=0, concat_axis=0, axis_index_groups=groups, tiled=True)
    return jnp.moveaxis(mine.astype(jnp.float32), 0, 1).reshape(template_ids.shape[0], bins)


def solution(mesh):
    in_specs = (P("tm", None, "freq"), P(), P(), P(), P("tm", None))
    out_specs = P("tm", "freq")
    return jax.shard_map(shards, mesh=mesh, in_specs=in_specs, out_specs=out_specs, check_vma=False)
```

```python
import functools
import math

import jax
import jax.numpy as jnp
from jax import lax
from jax.experimental import pallas as pl
from jax.experimental.pallas import tpu as pltpu
from jax.sharding import PartitionSpec as P

NBIN = 4096
LAGMAX = 16
NGRID = 64
PERIOD = 283
ROWS = 288
EROWS = ROWS + LAGMAX
LANES = 128
PARTS = 2
EXTRA = 8

SIN_COEF = (4.442883014678955, -7.308245658874512, 3.606354236602783, -0.8461116552352905, 0.1098245158791542)
COS_COEF = (1.4142135381698608, -6.978850841522217, 5.739460468292236, -1.883557915687561, 0.3106880187988281)


def horner(coef, y):
    total = coef[-1] * y + coef[-2]
    for value in coef[-3::-1]:
        total = total * y + value
    return total


def sincos_turns(x):
    f = x - jnp.round(x)
    y = f * f
    s = horner(SIN_COEF, y) * f
    c = horner(COS_COEF, y)
    return s * c, 1.0 - s * s


def send_kernel(shift_ref, sfts_ref, ids_ref, out_ref):
    rows = sfts_ref.shape[0]
    pieces = sfts_ref.shape[2] // LANES
    copies = out_ref.shape[0] // pieces
    squares = jnp.zeros((rows, LANES), jnp.float32)
    for c in range(2):
        for v in range(pieces):
            tile = sfts_ref[:, c, v * LANES : (v + 1) * LANES]
            squares = squares + tile * tile
            small = tile.astype(jnp.bfloat16)
            for u in range(copies):
                out_ref[u * pieces + v, c * rows : (c + 1) * rows, :] = small
    square = jnp.concatenate([squares, jnp.zeros((LANES - rows, LANES), jnp.float32)], 0)
    power = jnp.sum(square.T, axis=0, keepdims=True)
    power = pltpu.roll(power, shift_ref[0], 1)
    high = power.astype(jnp.bfloat16)
    rest = power - high.astype(jnp.float32)
    middle = rest.astype(jnp.bfloat16)
    low = (rest - middle.astype(jnp.float32)).astype(jnp.bfloat16)
    ids = ids_ref[...].astype(jnp.float32).astype(jnp.bfloat16)
    spare = jnp.zeros((EXTRA - 5, LANES), jnp.bfloat16)
    extra = jnp.concatenate([high, middle, low, ids, spare], 0)
    for d in range(out_ref.shape[0]):
        out_ref[d, 2 * rows :, :] = extra


def to_send(shift, sfts, ids, times):
    rows = sfts.shape[0]
    vmem = pl.BlockSpec(memory_space=pltpu.VMEM)
    return pl.pallas_call(
        send_kernel,
        out_shape=jax.ShapeDtypeStruct((times, 2 * rows + EXTRA, LANES), jnp.bfloat16),
        in_specs=[pl.BlockSpec(memory_space=pltpu.SMEM), vmem, vmem],
        out_specs=vmem,
        name="to_send",
    )(shift, sfts, ids)


def spread(line):
    return jnp.broadcast_to(line, (LANES, LANES)).T


def weight_kernel(total, lags_ref, inter_ref, det_ref, out_ref, det, near):
    lag = lags_ref[pl.program_id(0)]

    @pl.when(pl.program_id(0) == 0)
    def _():
        for g in range(total // LANES):
            column = spread(det_ref[g : g + 1, :].astype(jnp.float32))
            det[g * LANES : (g + 1) * LANES, :] = column
            for b in range(3):
                near[b, g * LANES : (g + 1) * LANES, :] = jnp.where(
                    column == 0.0, inter_ref[0, b], jnp.where(column == 1.0, inter_ref[1, b], inter_ref[2, b])
                )
        rest = det.shape[0] - total
        det[total:, :] = jnp.zeros((rest, LANES), jnp.float32)
        for b in range(3):
            near[b, total:, :] = jnp.zeros((rest, LANES), jnp.float32)

    for m in range(out_ref.shape[1]):
        for b in range(ROWS // 16):
            i0 = m * PERIOD + b * 16
            far = det[pl.ds(lag + i0, 16), :]
            out_ref[0, m, b * 16 : b * 16 + 16, :] = jnp.where(
                far == 0.0,
                near[0, i0 : i0 + 16, :],
                jnp.where(far == 1.0, near[1, i0 : i0 + 16, :], near[2, i0 : i0 + 16, :]),
            )


def weights(lags, intersection, det):
    total = det.size
    cycles = -(-total // PERIOD)
    smem = pl.BlockSpec(memory_space=pltpu.SMEM)
    length = PERIOD * cycles + ROWS + LAGMAX
    length = -(-length // 32) * 32 + 8
    count = lags.shape[0]
    return pl.pallas_call(
        functools.partial(weight_kernel, total),
        grid=(count,),
        out_shape=jax.ShapeDtypeStruct((count, cycles, ROWS, LANES), jnp.float32),
        in_specs=[smem, smem, pl.BlockSpec(det.shape, lambda l: (0, 0))],
        out_specs=pl.BlockSpec((1, cycles, ROWS, LANES), lambda l: (l, 0, 0, 0)),
        scratch_shapes=[pltpu.VMEM((length, LANES), jnp.float32), pltpu.VMEM((3, length, LANES), jnp.float32)],
        cost_estimate=pl.CostEstimate(
            flops=1000 * count * cycles * ROWS * LANES,
            bytes_accessed=4 * count * cycles * ROWS * LANES,
            transcendentals=0,
        ),
        name="weights",
    )(lags, intersection, det)


def stat_kernel(
    scale,
    total,
    lags_ref,
    first_ref,
    every_ref,
    power_ref,
    weight_hbm,
    out_ref,
    z,
    fold,
    pairs,
    sa,
    ca,
    far,
    near,
    weight,
    sems,
):
    lag_count = lags_ref.shape[0]
    devices, rows, _ = every_ref.shape
    rows = (rows - EXTRA) // 2
    blocks = out_ref.shape[0]
    parts = sems.shape[0]
    group = lag_count // parts
    copies = [
        pltpu.make_async_copy(
            weight_hbm.at[p * group : (p + 1) * group], weight.at[p * group : (p + 1) * group], sems.at[p]
        )
        for p in range(parts)
    ]
    for copy in copies:
        copy.start()

    powers = power_ref[0]
    for q in range(1, power_ref.shape[0]):
        powers = powers + power_ref[q]
    factor_of = lax.rsqrt(powers * (1.0 / NBIN) + 1e-06)
    lane = lax.broadcasted_iota(jnp.int32, (1, LANES), 1)
    for g in range(total // LANES):
        first = g * LANES // rows
        last = (g * LANES + LANES - 1) // rows
        line = factor_of[first : first + 1]
        for d in range(first + 1, last + 1):
            line = jnp.where(lane < d * rows - g * LANES, line, factor_of[d : d + 1])
        column = spread(line)
        for h in range(LANES // 16):
            i0 = g * LANES + h * 16
            d, r = divmod(i0, rows)
            for c in range(2):
                raw = every_ref[d, c * rows + r : c * rows + r + 16, :].astype(jnp.float32)
                z[c, i0 : i0 + 16, :] = raw * column[h * 16 : h * 16 + 16]
    rest = z.shape[1] - total
    for c in range(2):
        z[c, total:, :] = jnp.zeros((rest, LANES), jnp.float32)

    for b in range(EROWS // 16):
        r0 = b * 16
        row = lax.broadcasted_iota(jnp.int32, (16, LANES), 0) + r0
        s, c = sincos_turns(row.astype(jnp.float32) * (1.0 / PERIOD))
        sa[r0 : r0 + 16, :] = s
        ca[r0 : r0 + 16, :] = c

    def exp_block(t, carry):
        ids = every_ref[first_ref[0] + t, 2 * rows : 2 * rows + EXTRA, :].astype(jnp.float32)
        amplitude = (8.0 + 4.0 * ids[3:4]) * (1.0 / (2.0 * math.pi))
        sq, cq = sincos_turns(ids[4:5] * (1.0 / NGRID))
        with_sin = jnp.broadcast_to(amplitude * cq, (16, LANES))
        with_cos = jnp.broadcast_to(amplitude * sq, (16, LANES))
        for b in range(EROWS // 16):
            r0 = b * 16
            s, c = sincos_turns(sa[r0 : r0 + 16, :] * with_sin + ca[r0 : r0 + 16, :] * with_cos)
            far[t, 0, r0 : r0 + 16, :] = c
            far[t, 1, r0 : r0 + 16, :] = s
            if r0 < ROWS:
                near[t, 0, r0 : r0 + 16, :] = c.astype(jnp.bfloat16)
                near[t, 1, r0 : r0 + 16, :] = s.astype(jnp.bfloat16)
        return carry

    lax.fori_loop(0, blocks, exp_block, 0)

    def pair_block(lags_here, cycles, b, carry):
        r0 = pl.multiple_of(b * 16, 16)
        lag = {l: lags_ref[l] for l in lags_here}
        acc = {}
        for m in range(cycles):
            i0 = r0 + PERIOD * m
            a = z[0, pl.ds(i0, 16), :]
            bb = z[1, pl.ds(i0, 16), :]
            for l in lags_here:
                j0 = i0 + lag[l]
                w = weight[l, m, pl.ds(r0, 16), :]
                c = w * z[0, pl.ds(j0, 16), :]
                d = w * z[1, pl.ds(j0, 16), :]
                re = a * c + bb * d
                im = a * d - bb * c
                acc[l] = (re, im) if m == 0 else (acc[l][0] + re, acc[l][1] + im)
        at = pl.multiple_of(b * 32, 16)
        for l in lags_here:
            fold[pl.ds(pl.multiple_of(2 * l * ROWS + at, 16), 16), :] = acc[l][0]
            fold[pl.ds(pl.multiple_of(2 * l * ROWS + 16 + at, 16), 16), :] = acc[l][1]
        return carry

    full = total // PERIOD
    split = -(-(total - full * PERIOD) // 16)
    for p in range(parts):
        copies[p].wait()
        here = range(p * group, (p + 1) * group)
        lax.fori_loop(0, split, functools.partial(pair_block, here, full + 1), 0)
        lax.fori_loop(split, ROWS // 16, functools.partial(pair_block, here, full), 0)
    for l in range(lag_count):
        for c in range(2):
            at = 2 * (l + 1) * ROWS - 16 * (1 - c) - (ROWS - PERIOD)
            fold[at : at + ROWS - PERIOD, :] = jnp.zeros((ROWS - PERIOD, LANES), jnp.float32)

    wide = 4
    deep = 256
    spans = ROWS // 16
    lag = [lags_ref[l] for l in range(lag_count)]
    sums = [None] * (blocks // wide)
    for k in range(2 * lag_count * ROWS // deep):
        for b in range(deep // LANES):
            at = k * deep + b * LANES
            pairs[:, at : at + LANES] = fold[at : at + LANES, :].T.astype(jnp.bfloat16)
        for n in range(blocks // wide):
            columns = []
            for t in range(n * wide, (n + 1) * wide):
                column = []
                for q in range(k * deep // 32, (k + 1) * deep // 32):
                    l, b = divmod(q, spans)
                    r0 = b * 16
                    cr = near[t, 0, r0 : r0 + 16, :]
                    ci = near[t, 1, r0 : r0 + 16, :]
                    fr = far[t, 0, pl.ds(lag[l] + r0, 16), :].astype(jnp.bfloat16)
                    fi = far[t, 1, pl.ds(lag[l] + r0, 16), :].astype(jnp.bfloat16)
                    column += [fr * cr + fi * ci, fi * cr - fr * ci]
                columns.append(jnp.concatenate(column, 0))
            term = jnp.dot(
                pairs[:, k * deep : (k + 1) * deep],
                jnp.concatenate(columns, 1),
                preferred_element_type=jnp.float32,
            )
            sums[n] = term if k == 0 else sums[n] + term
    for n in range(blocks // wide):
        for h in range(wide):
            out_ref[n * wide + h] = (sums[n][:, h * LANES : (h + 1) * LANES] * scale).T.astype(jnp.bfloat16)


def statistic(lags, first, every, power, weight, blocks, scale, total):
    depth = 2 * lags.shape[0] * ROWS
    reach = PERIOD * (total // PERIOD) + ROWS + LAGMAX
    zrows = -(-reach // 32) * 32 + 24
    smem = pl.BlockSpec(memory_space=pltpu.SMEM)
    vmem = pl.BlockSpec(memory_space=pltpu.VMEM)
    f32 = jnp.float32
    return pl.pallas_call(
        functools.partial(stat_kernel, scale, total),
        out_shape=jax.ShapeDtypeStruct((blocks, LANES, LANES), jnp.bfloat16),
        in_specs=[smem, smem, vmem, vmem, pl.BlockSpec(memory_space=pl.ANY)],
        out_specs=vmem,
        scratch_shapes=[
            pltpu.VMEM((2, zrows, LANES), f32),
            pltpu.VMEM((depth, LANES), f32),
            pltpu.VMEM((LANES, depth), jnp.bfloat16),
            pltpu.VMEM((EROWS, LANES), f32),
            pltpu.VMEM((EROWS, LANES), f32),
            pltpu.VMEM((blocks, 2, EROWS, LANES), f32),
            pltpu.VMEM((blocks, 2, ROWS, LANES), jnp.bfloat16),
            pltpu.VMEM(weight.shape, f32),
            pltpu.SemaphoreType.DMA((PARTS,)),
        ],
        cost_estimate=pl.CostEstimate(
            flops=2 * depth * blocks * LANES * LANES, bytes_accessed=every.size * 2, transcendentals=0
        ),
        name="statistic",
    )(lags, first, every, power, weight)


def shards(sfts, detector_ids, intersection, lags, template_ids):
    rows, _, bins = sfts.shape
    times = lax.axis_size("tm")
    quarters = lax.axis_size("freq")
    pieces = bins // LANES
    groups = [list(range(g, g + pieces)) for g in range(0, times, pieces)]
    total = detector_ids.shape[0]
    scale = 1.0 / math.sqrt(total * lags.shape[0])
    place = lax.axis_index("tm").astype(jnp.int32)

    send = to_send((place * rows % LANES)[None], sfts, template_ids.T, times)
    every = lax.all_to_all(send, "tm", split_axis=0, concat_axis=0, tiled=True)
    weight = weights(lags, intersection, detector_ids.reshape(total // LANES, LANES))
    every, place, weight = lax.optimization_barrier((every, place, weight))

    power = every[:, 2 * rows : 2 * rows + 3].astype(jnp.float32).sum(axis=1)
    power = lax.all_gather(power, "freq", axis=0, tiled=True).reshape(quarters, *power.shape)
    first = (place // pieces * pieces)[None]
    part = statistic(lags, first, every, power, weight, pieces, scale, total)
    mine = lax.all_to_all(part, "tm", split_axis=0, concat_axis=0, axis_index_groups=groups, tiled=True)
    return jnp.moveaxis(mine.astype(jnp.float32), 0, 1).reshape(template_ids.shape[0], bins)


def solution(mesh):
    in_specs = (P("tm", None, "freq"), P(), P(), P(), P("tm", None))
    out_specs = P("tm", "freq")
    return jax.shard_map(shards, mesh=mesh, in_specs=in_specs, out_specs=out_specs, check_vma=False)
```

```python
import functools
import math

import jax
import jax.numpy as jnp
from jax import lax
from jax.experimental import pallas as pl
from jax.experimental.pallas import tpu as pltpu
from jax.sharding import PartitionSpec as P

NBIN = 4096
LAGMAX = 16
NGRID = 64
PERIOD = 283
ROWS = 288
EROWS = ROWS + LAGMAX
LANES = 128
PARTS = 2
EXTRA = 8

SIN_COEF = (4.442883014678955, -7.308245658874512, 3.606354236602783, -0.8461116552352905, 0.1098245158791542)
COS_COEF = (1.4142135381698608, -6.978850841522217, 5.739460468292236, -1.883557915687561, 0.3106880187988281)


def horner(coef, y):
    total = coef[-1] * y + coef[-2]
    for value in coef[-3::-1]:
        total = total * y + value
    return total


def sincos_turns(x):
    f = x - jnp.round(x)
    y = f * f
    s = horner(SIN_COEF, y) * f
    c = horner(COS_COEF, y)
    return s * c, 1.0 - s * s


def send_kernel(shift_ref, sfts_ref, ids_ref, out_ref):
    rows = sfts_ref.shape[0]
    pieces = sfts_ref.shape[2] // LANES
    copies = out_ref.shape[0] // pieces
    squares = jnp.zeros((rows, LANES), jnp.float32)
    for c in range(2):
        for v in range(pieces):
            tile = sfts_ref[:, c, v * LANES : (v + 1) * LANES]
            squares = squares + tile * tile
            small = tile.astype(jnp.bfloat16)
            for u in range(copies):
                out_ref[u * pieces + v, c * rows : (c + 1) * rows, :] = small
    square = jnp.concatenate([squares, jnp.zeros((LANES - rows, LANES), jnp.float32)], 0)
    power = jnp.sum(square.T, axis=0, keepdims=True)
    power = pltpu.roll(power, shift_ref[0], 1)
    high = power.astype(jnp.bfloat16)
    rest = power - high.astype(jnp.float32)
    middle = rest.astype(jnp.bfloat16)
    low = (rest - middle.astype(jnp.float32)).astype(jnp.bfloat16)
    ids = ids_ref[...].astype(jnp.float32).astype(jnp.bfloat16)
    spare = jnp.zeros((EXTRA - 5, LANES), jnp.bfloat16)
    extra = jnp.concatenate([high, middle, low, ids, spare], 0)
    for d in range(out_ref.shape[0]):
        out_ref[d, 2 * rows :, :] = extra


def to_send(shift, sfts, ids, times):
    rows = sfts.shape[0]
    vmem = pl.BlockSpec(memory_space=pltpu.VMEM)
    return pl.pallas_call(
        send_kernel,
        out_shape=jax.ShapeDtypeStruct((times, 2 * rows + EXTRA, LANES), jnp.bfloat16),
        in_specs=[pl.BlockSpec(memory_space=pltpu.SMEM), vmem, vmem],
        out_specs=vmem,
        name="to_send",
    )(shift, sfts, ids)


def spread(line):
    return jnp.broadcast_to(line, (LANES, LANES)).T


def weight_kernel(total, lags_ref, inter_ref, det_ref, out_ref, det, near):
    lag = lags_ref[pl.program_id(0)]

    @pl.when(pl.program_id(0) == 0)
    def _():
        for g in range(total // LANES):
            column = spread(det_ref[g : g + 1, :].astype(jnp.float32))
            det[g * LANES : (g + 1) * LANES, :] = column
            for b in range(3):
                near[b, g * LANES : (g + 1) * LANES, :] = jnp.where(
                    column == 0.0, inter_ref[0, b], jnp.where(column == 1.0, inter_ref[1, b], inter_ref[2, b])
                )
        rest = det.shape[0] - total
        det[total:, :] = jnp.zeros((rest, LANES), jnp.float32)
        for b in range(3):
            near[b, total:, :] = jnp.zeros((rest, LANES), jnp.float32)

    for m in range(out_ref.shape[1]):
        for b in range(ROWS // 16):
            i0 = m * PERIOD + b * 16
            far = det[pl.ds(lag + i0, 16), :]
            out_ref[0, m, b * 16 : b * 16 + 16, :] = jnp.where(
                far == 0.0,
                near[0, i0 : i0 + 16, :],
                jnp.where(far == 1.0, near[1, i0 : i0 + 16, :], near[2, i0 : i0 + 16, :]),
            ).astype(jnp.bfloat16)


def weights(lags, intersection, det):
    total = det.size
    cycles = -(-total // PERIOD)
    smem = pl.BlockSpec(memory_space=pltpu.SMEM)
    length = PERIOD * cycles + ROWS + LAGMAX
    length = -(-length // 32) * 32 + 8
    count = lags.shape[0]
    return pl.pallas_call(
        functools.partial(weight_kernel, total),
        grid=(count,),
        out_shape=jax.ShapeDtypeStruct((count, cycles, ROWS, LANES), jnp.bfloat16),
        in_specs=[smem, smem, pl.BlockSpec(det.shape, lambda l: (0, 0))],
        out_specs=pl.BlockSpec((1, cycles, ROWS, LANES), lambda l: (l, 0, 0, 0)),
        scratch_shapes=[pltpu.VMEM((length, LANES), jnp.float32), pltpu.VMEM((3, length, LANES), jnp.float32)],
        cost_estimate=pl.CostEstimate(
            flops=1000 * count * cycles * ROWS * LANES,
            bytes_accessed=2 * count * cycles * ROWS * LANES,
            transcendentals=0,
        ),
        name="weights",
    )(lags, intersection, det)


def stat_kernel(
    scale,
    total,
    lags_ref,
    first_ref,
    every_ref,
    power_ref,
    weight_hbm,
    out_ref,
    z,
    fold,
    pairs,
    sa,
    ca,
    far,
    near,
    weight,
    sems,
):
    lag_count = lags_ref.shape[0]
    devices, rows, _ = every_ref.shape
    rows = (rows - EXTRA) // 2
    blocks = out_ref.shape[0]
    parts = sems.shape[0]
    group = lag_count // parts
    copies = [
        pltpu.make_async_copy(
            weight_hbm.at[p * group : (p + 1) * group], weight.at[p * group : (p + 1) * group], sems.at[p]
        )
        for p in range(parts)
    ]
    for copy in copies:
        copy.start()

    powers = power_ref[0]
    for q in range(1, power_ref.shape[0]):
        powers = powers + power_ref[q]
    factor_of = lax.rsqrt(powers * (1.0 / NBIN) + 1e-06)
    lane = lax.broadcasted_iota(jnp.int32, (1, LANES), 1)
    for g in range(total // LANES):
        first = g * LANES // rows
        last = (g * LANES + LANES - 1) // rows
        line = factor_of[first : first + 1]
        for d in range(first + 1, last + 1):
            line = jnp.where(lane < d * rows - g * LANES, line, factor_of[d : d + 1])
        column = spread(line)
        for h in range(LANES // 16):
            i0 = g * LANES + h * 16
            d, r = divmod(i0, rows)
            for c in range(2):
                raw = every_ref[d, c * rows + r : c * rows + r + 16, :].astype(jnp.float32)
                z[c, i0 : i0 + 16, :] = raw * column[h * 16 : h * 16 + 16]
    rest = z.shape[1] - total
    for c in range(2):
        z[c, total:, :] = jnp.zeros((rest, LANES), jnp.float32)

    for b in range(EROWS // 16):
        r0 = b * 16
        row = lax.broadcasted_iota(jnp.int32, (16, LANES), 0) + r0
        s, c = sincos_turns(row.astype(jnp.float32) * (1.0 / PERIOD))
        sa[r0 : r0 + 16, :] = s
        ca[r0 : r0 + 16, :] = c

    def exp_block(t, carry):
        ids = every_ref[first_ref[0] + t, 2 * rows : 2 * rows + EXTRA, :].astype(jnp.float32)
        amplitude = (8.0 + 4.0 * ids[3:4]) * (1.0 / (2.0 * math.pi))
        sq, cq = sincos_turns(ids[4:5] * (1.0 / NGRID))
        with_sin = jnp.broadcast_to(amplitude * cq, (16, LANES))
        with_cos = jnp.broadcast_to(amplitude * sq, (16, LANES))
        for b in range(EROWS // 16):
            r0 = b * 16
            s, c = sincos_turns(sa[r0 : r0 + 16, :] * with_sin + ca[r0 : r0 + 16, :] * with_cos)
            far[t, 0, r0 : r0 + 16, :] = c
            far[t, 1, r0 : r0 + 16, :] = s
            if r0 < ROWS:
                near[t, 0, r0 : r0 + 16, :] = c.astype(jnp.bfloat16)
                near[t, 1, r0 : r0 + 16, :] = s.astype(jnp.bfloat16)
        return carry

    lax.fori_loop(0, blocks, exp_block, 0)

    def pair_block(lags_here, cycles, b, carry):
        r0 = pl.multiple_of(b * 16, 16)
        lag = {l: lags_ref[l] for l in lags_here}
        acc = {}
        for m in range(cycles):
            i0 = r0 + PERIOD * m
            a = z[0, pl.ds(i0, 16), :]
            bb = z[1, pl.ds(i0, 16), :]
            for l in lags_here:
                j0 = i0 + lag[l]
                w = weight[l, m, pl.ds(r0, 16), :].astype(jnp.float32)
                c = w * z[0, pl.ds(j0, 16), :]
                d = w * z[1, pl.ds(j0, 16), :]
                re = a * c + bb * d
                im = a * d - bb * c
                acc[l] = (re, im) if m == 0 else (acc[l][0] + re, acc[l][1] + im)
        for l in lags_here:
            for c in range(2):
                fold[b * lag_count + l, c * 16 : c * 16 + 16, :] = acc[l][c]
        return carry

    full = total // PERIOD
    split = -(-(total - full * PERIOD) // 16)
    for p in range(parts):
        copies[p].wait()
        here = range(p * group, (p + 1) * group)
        lax.fori_loop(0, split, functools.partial(pair_block, here, full + 1), 0)
        lax.fori_loop(split, ROWS // 16, functools.partial(pair_block, here, full), 0)
    spans = ROWS // 16
    kept = lax.broadcasted_iota(jnp.int32, (16, LANES), 0) < PERIOD - (spans - 1) * 16
    for l in range(lag_count):
        for c in range(2):
            q = (spans - 1) * lag_count + l
            value = fold[q, c * 16 : c * 16 + 16, :].astype(jnp.float32)
            fold[q, c * 16 : c * 16 + 16, :] = jnp.where(kept, value, 0.0)

    wide = 4
    deep = 256
    lag = [lags_ref[l] for l in range(lag_count)]
    sums = [None] * (blocks // wide)
    for k in range(2 * lag_count * ROWS // deep):
        for b in range(deep // LANES):
            at = k * deep + b * LANES
            tile = fold[at // 32 : at // 32 + LANES // 32].reshape(LANES, LANES)
            pairs[:, at : at + LANES] = tile.T.astype(jnp.bfloat16)
        for n in range(blocks // wide):
            columns = []
            for t in range(n * wide, (n + 1) * wide):
                column = []
                for q in range(k * deep // 32, (k + 1) * deep // 32):
                    b, l = divmod(q, lag_count)
                    r0 = b * 16
                    cr = near[t, 0, r0 : r0 + 16, :]
                    ci = near[t, 1, r0 : r0 + 16, :]
                    fr = far[t, 0, pl.ds(lag[l] + r0, 16), :].astype(jnp.bfloat16)
                    fi = far[t, 1, pl.ds(lag[l] + r0, 16), :].astype(jnp.bfloat16)
                    column += [fr * cr + fi * ci, fi * cr - fr * ci]
                columns.append(jnp.concatenate(column, 0))
            term = jnp.dot(
                pairs[:, k * deep : (k + 1) * deep],
                jnp.concatenate(columns, 1),
                preferred_element_type=jnp.float32,
            )
            sums[n] = term if k == 0 else sums[n] + term
    for n in range(blocks // wide):
        for h in range(wide):
            out_ref[n * wide + h] = (sums[n][:, h * LANES : (h + 1) * LANES] * scale).T.astype(jnp.bfloat16)


def statistic(lags, first, every, power, weight, blocks, scale, total):
    depth = 2 * lags.shape[0] * ROWS
    reach = PERIOD * (total // PERIOD) + ROWS + LAGMAX
    zrows = -(-reach // 32) * 32 + 16
    smem = pl.BlockSpec(memory_space=pltpu.SMEM)
    vmem = pl.BlockSpec(memory_space=pltpu.VMEM)
    f32 = jnp.float32
    return pl.pallas_call(
        functools.partial(stat_kernel, scale, total),
        out_shape=jax.ShapeDtypeStruct((blocks, LANES, LANES), jnp.bfloat16),
        in_specs=[smem, smem, vmem, vmem, pl.BlockSpec(memory_space=pl.ANY)],
        out_specs=vmem,
        scratch_shapes=[
            pltpu.VMEM((2, zrows, LANES), f32),
            pltpu.VMEM((depth // 32, 32, LANES), f32),
            pltpu.VMEM((LANES, depth), jnp.bfloat16),
            pltpu.VMEM((EROWS, LANES), f32),
            pltpu.VMEM((EROWS, LANES), f32),
            pltpu.VMEM((blocks, 2, EROWS, LANES), f32),
            pltpu.VMEM((blocks, 2, ROWS, LANES), jnp.bfloat16),
            pltpu.VMEM(weight.shape, weight.dtype),
            pltpu.SemaphoreType.DMA((PARTS,)),
        ],
        cost_estimate=pl.CostEstimate(
            flops=2 * depth * blocks * LANES * LANES, bytes_accessed=every.size * 2, transcendentals=0
        ),
        name="statistic",
    )(lags, first, every, power, weight)


def shards(sfts, detector_ids, intersection, lags, template_ids):
    rows, _, bins = sfts.shape
    times = lax.axis_size("tm")
    quarters = lax.axis_size("freq")
    pieces = bins // LANES
    groups = [list(range(g, g + pieces)) for g in range(0, times, pieces)]
    total = detector_ids.shape[0]
    scale = 1.0 / math.sqrt(total * lags.shape[0])
    place = lax.axis_index("tm").astype(jnp.int32)

    send = to_send((place * rows % LANES)[None], sfts, template_ids.T, times)
    every = lax.all_to_all(send, "tm", split_axis=0, concat_axis=0, tiled=True)
    weight = weights(lags, intersection, detector_ids.reshape(total // LANES, LANES))
    every, place, weight = lax.optimization_barrier((every, place, weight))

    power = every[:, 2 * rows : 2 * rows + 3].astype(jnp.float32).sum(axis=1)
    power = lax.all_gather(power, "freq", axis=0, tiled=True).reshape(quarters, *power.shape)
    first = (place // pieces * pieces)[None]
    part = statistic(lags, first, every, power, weight, pieces, scale, total)
    mine = lax.all_to_all(part, "tm", split_axis=0, concat_axis=0, axis_index_groups=groups, tiled=True)
    return jnp.moveaxis(mine.astype(jnp.float32), 0, 1).reshape(template_ids.shape[0], bins)


def solution(mesh):
    in_specs = (P("tm", None, "freq"), P(), P(), P(), P("tm", None))
    out_specs = P("tm", "freq")
    return jax.shard_map(shards, mesh=mesh, in_specs=in_specs, out_specs=out_specs, check_vma=False)
```

```python
import functools
import math

import jax
import jax.numpy as jnp
from jax import lax
from jax.experimental import pallas as pl
from jax.experimental.pallas import tpu as pltpu
from jax.sharding import PartitionSpec as P

NBIN = 4096
LAGMAX = 16
NGRID = 64
PERIOD = 283
ROWS = 288
EROWS = ROWS + LAGMAX
LANES = 128
PARTS = 2
EXTRA = 8

SIN_COEF = (4.442883014678955, -7.308245658874512, 3.606354236602783, -0.8461116552352905, 0.1098245158791542)
COS_COEF = (1.4142135381698608, -6.978850841522217, 5.739460468292236, -1.883557915687561, 0.3106880187988281)


def horner(coef, y):
    total = coef[-1] * y + coef[-2]
    for value in coef[-3::-1]:
        total = total * y + value
    return total


def sincos_turns(x):
    f = x - jnp.round(x)
    y = f * f
    s = horner(SIN_COEF, y) * f
    c = horner(COS_COEF, y)
    return s * c, 1.0 - s * s


def send_kernel(shift_ref, sfts_ref, ids_ref, out_ref):
    rows = sfts_ref.shape[0]
    pieces = sfts_ref.shape[2] // LANES
    copies = out_ref.shape[0] // pieces
    squares = jnp.zeros((rows, LANES), jnp.float32)
    for c in range(2):
        for v in range(pieces):
            tile = sfts_ref[:, c, v * LANES : (v + 1) * LANES]
            squares = squares + tile * tile
            small = tile.astype(jnp.bfloat16)
            for u in range(copies):
                out_ref[u * pieces + v, c * rows : (c + 1) * rows, :] = small
    square = jnp.concatenate([squares, jnp.zeros((LANES - rows, LANES), jnp.float32)], 0)
    power = jnp.sum(square.T, axis=0, keepdims=True)
    power = pltpu.roll(power, shift_ref[0], 1)
    high = power.astype(jnp.bfloat16)
    rest = power - high.astype(jnp.float32)
    middle = rest.astype(jnp.bfloat16)
    low = (rest - middle.astype(jnp.float32)).astype(jnp.bfloat16)
    ids = ids_ref[...].astype(jnp.float32).astype(jnp.bfloat16)
    spare = jnp.zeros((EXTRA - 5, LANES), jnp.bfloat16)
    extra = jnp.concatenate([high, middle, low, ids, spare], 0)
    for d in range(out_ref.shape[0]):
        out_ref[d, 2 * rows :, :] = extra


def to_send(shift, sfts, ids, times):
    rows = sfts.shape[0]
    vmem = pl.BlockSpec(memory_space=pltpu.VMEM)
    return pl.pallas_call(
        send_kernel,
        out_shape=pltpu.VMEM((times, 2 * rows + EXTRA, LANES), jnp.bfloat16),
        in_specs=[pl.BlockSpec(memory_space=pltpu.SMEM), vmem, vmem],
        out_specs=vmem,
        name="to_send",
    )(shift, sfts, ids)


def spread(line):
    return jnp.broadcast_to(line, (LANES, LANES)).T


def weight_kernel(total, lags_ref, inter_ref, det_ref, out_ref, det, near):
    lag = lags_ref[pl.program_id(0)]

    @pl.when(pl.program_id(0) == 0)
    def _():
        for g in range(total // LANES):
            column = spread(det_ref[g : g + 1, :].astype(jnp.float32))
            det[g * LANES : (g + 1) * LANES, :] = column
            for b in range(3):
                near[b, g * LANES : (g + 1) * LANES, :] = jnp.where(
                    column == 0.0, inter_ref[0, b], jnp.where(column == 1.0, inter_ref[1, b], inter_ref[2, b])
                )
        rest = det.shape[0] - total
        det[total:, :] = jnp.zeros((rest, LANES), jnp.float32)
        for b in range(3):
            near[b, total:, :] = jnp.zeros((rest, LANES), jnp.float32)

    for m in range(out_ref.shape[1]):
        for b in range(ROWS // 16):
            i0 = m * PERIOD + b * 16
            far = det[pl.ds(lag + i0, 16), :]
            out_ref[0, m, b * 16 : b * 16 + 16, :] = jnp.where(
                far == 0.0,
                near[0, i0 : i0 + 16, :],
                jnp.where(far == 1.0, near[1, i0 : i0 + 16, :], near[2, i0 : i0 + 16, :]),
            ).astype(jnp.bfloat16)


def weights(lags, intersection, det):
    total = det.size
    cycles = -(-total // PERIOD)
    smem = pl.BlockSpec(memory_space=pltpu.SMEM)
    length = PERIOD * cycles + ROWS + LAGMAX
    length = -(-length // 32) * 32 + 8
    count = lags.shape[0]
    return pl.pallas_call(
        functools.partial(weight_kernel, total),
        grid=(count,),
        out_shape=jax.ShapeDtypeStruct((count, cycles, ROWS, LANES), jnp.bfloat16),
        in_specs=[smem, smem, pl.BlockSpec(det.shape, lambda l: (0, 0))],
        out_specs=pl.BlockSpec((1, cycles, ROWS, LANES), lambda l: (l, 0, 0, 0)),
        scratch_shapes=[pltpu.VMEM((length, LANES), jnp.float32), pltpu.VMEM((3, length, LANES), jnp.float32)],
        cost_estimate=pl.CostEstimate(
            flops=1000 * count * cycles * ROWS * LANES,
            bytes_accessed=2 * count * cycles * ROWS * LANES,
            transcendentals=0,
        ),
        name="weights",
    )(lags, intersection, det)


def stat_kernel(
    scale,
    total,
    lags_ref,
    first_ref,
    every_ref,
    power_ref,
    weight_hbm,
    out_ref,
    z,
    fold,
    sa,
    ca,
    far,
    near,
    weight,
    sems,
):
    lag_count = lags_ref.shape[0]
    devices, rows, _ = every_ref.shape
    rows = (rows - EXTRA) // 2
    blocks = out_ref.shape[0]
    parts = sems.shape[0]
    group = lag_count // parts
    copies = [
        pltpu.make_async_copy(
            weight_hbm.at[p * group : (p + 1) * group], weight.at[p * group : (p + 1) * group], sems.at[p]
        )
        for p in range(parts)
    ]
    for copy in copies:
        copy.start()

    powers = power_ref[0]
    for q in range(1, power_ref.shape[0]):
        powers = powers + power_ref[q]
    factor_of = lax.rsqrt(powers * (1.0 / NBIN) + 1e-06)
    lane = lax.broadcasted_iota(jnp.int32, (1, LANES), 1)
    for g in range(total // LANES):
        first = g * LANES // rows
        last = (g * LANES + LANES - 1) // rows
        line = factor_of[first : first + 1]
        for d in range(first + 1, last + 1):
            line = jnp.where(lane < d * rows - g * LANES, line, factor_of[d : d + 1])
        column = spread(line)
        for h in range(LANES // 16):
            i0 = g * LANES + h * 16
            d, r = divmod(i0, rows)
            for c in range(2):
                raw = every_ref[d, c * rows + r : c * rows + r + 16, :].astype(jnp.float32)
                z[c, i0 : i0 + 16, :] = raw * column[h * 16 : h * 16 + 16]
    rest = z.shape[1] - total
    for c in range(2):
        z[c, total:, :] = jnp.zeros((rest, LANES), jnp.float32)

    for b in range(EROWS // 16):
        r0 = b * 16
        row = lax.broadcasted_iota(jnp.int32, (16, LANES), 0) + r0
        s, c = sincos_turns(row.astype(jnp.float32) * (1.0 / PERIOD))
        sa[r0 : r0 + 16, :] = s
        ca[r0 : r0 + 16, :] = c

    def exp_block(t, carry):
        ids = every_ref[first_ref[0] + t, 2 * rows : 2 * rows + EXTRA, :].astype(jnp.float32)
        amplitude = (8.0 + 4.0 * ids[3:4]) * (1.0 / (2.0 * math.pi))
        sq, cq = sincos_turns(ids[4:5] * (1.0 / NGRID))
        with_sin = jnp.broadcast_to(amplitude * cq, (16, LANES))
        with_cos = jnp.broadcast_to(amplitude * sq, (16, LANES))
        for b in range(EROWS // 16):
            r0 = b * 16
            s, c = sincos_turns(sa[r0 : r0 + 16, :] * with_sin + ca[r0 : r0 + 16, :] * with_cos)
            far[t, 0, r0 : r0 + 16, :] = c
            far[t, 1, r0 : r0 + 16, :] = s
            if r0 < ROWS:
                near[t, 0, r0 : r0 + 16, :] = c.astype(jnp.bfloat16)
                near[t, 1, r0 : r0 + 16, :] = s.astype(jnp.bfloat16)
        return carry

    lax.fori_loop(0, blocks, exp_block, 0)

    def pair_block(lags_here, cycles, b, carry):
        r0 = pl.multiple_of(b * 16, 16)
        lag = {l: lags_ref[l] for l in lags_here}
        acc = {}
        for m in range(cycles):
            i0 = r0 + PERIOD * m
            a = z[0, pl.ds(i0, 16), :]
            bb = z[1, pl.ds(i0, 16), :]
            for l in lags_here:
                j0 = i0 + lag[l]
                w = weight[l, m, pl.ds(r0, 16), :].astype(jnp.float32)
                c = w * z[0, pl.ds(j0, 16), :]
                d = w * z[1, pl.ds(j0, 16), :]
                re = a * c + bb * d
                im = a * d - bb * c
                acc[l] = (re, im) if m == 0 else (acc[l][0] + re, acc[l][1] + im)
        for l in lags_here:
            for c in range(2):
                fold[b * lag_count + l, c * 16 : c * 16 + 16, :] = acc[l][c]
        return carry

    full = total // PERIOD
    split = -(-(total - full * PERIOD) // 16)
    for p in range(parts):
        copies[p].wait()
        here = range(p * group, (p + 1) * group)
        lax.fori_loop(0, split, functools.partial(pair_block, here, full + 1), 0)
        lax.fori_loop(split, ROWS // 16, functools.partial(pair_block, here, full), 0)
    spans = ROWS // 16
    kept = lax.broadcasted_iota(jnp.int32, (16, LANES), 0) < PERIOD - (spans - 1) * 16
    for l in range(lag_count):
        for c in range(2):
            q = (spans - 1) * lag_count + l
            value = fold[q, c * 16 : c * 16 + 16, :].astype(jnp.float32)
            fold[q, c * 16 : c * 16 + 16, :] = jnp.where(kept, value, 0.0)

    wide = 4
    deep = 256
    lag = [lags_ref[l] for l in range(lag_count)]
    sums = [None] * (blocks // wide)
    for k in range(2 * lag_count * ROWS // deep):
        tile = fold[k * deep // 32 : (k + 1) * deep // 32].reshape(deep, LANES).astype(jnp.bfloat16)
        for n in range(blocks // wide):
            columns = []
            for t in range(n * wide, (n + 1) * wide):
                column = []
                for q in range(k * deep // 32, (k + 1) * deep // 32):
                    b, l = divmod(q, lag_count)
                    r0 = b * 16
                    cr = near[t, 0, r0 : r0 + 16, :]
                    ci = near[t, 1, r0 : r0 + 16, :]
                    fr = far[t, 0, pl.ds(lag[l] + r0, 16), :].astype(jnp.bfloat16)
                    fi = far[t, 1, pl.ds(lag[l] + r0, 16), :].astype(jnp.bfloat16)
                    column += [fr * cr + fi * ci, fi * cr - fr * ci]
                columns.append(jnp.concatenate(column, 0))
            term = lax.dot_general(
                tile,
                jnp.concatenate(columns, 1),
                (((0,), (0,)), ((), ())),
                preferred_element_type=jnp.float32,
            )
            sums[n] = term if k == 0 else sums[n] + term
    for n in range(blocks // wide):
        for h in range(wide):
            out_ref[n * wide + h] = (sums[n][:, h * LANES : (h + 1) * LANES] * scale).T.astype(jnp.bfloat16)


def statistic(lags, first, every, power, weight, blocks, scale, total):
    depth = 2 * lags.shape[0] * ROWS
    reach = PERIOD * (total // PERIOD) + ROWS + LAGMAX
    zrows = -(-reach // 32) * 32 + 16
    smem = pl.BlockSpec(memory_space=pltpu.SMEM)
    vmem = pl.BlockSpec(memory_space=pltpu.VMEM)
    f32 = jnp.float32
    return pl.pallas_call(
        functools.partial(stat_kernel, scale, total),
        out_shape=pltpu.VMEM((blocks, LANES, LANES), jnp.bfloat16),
        in_specs=[smem, smem, vmem, vmem, pl.BlockSpec(memory_space=pl.ANY)],
        out_specs=vmem,
        scratch_shapes=[
            pltpu.VMEM((2, zrows, LANES), f32),
            pltpu.VMEM((depth // 32, 32, LANES), f32),
            pltpu.VMEM((EROWS, LANES), f32),
            pltpu.VMEM((EROWS, LANES), f32),
            pltpu.VMEM((blocks, 2, EROWS, LANES), f32),
            pltpu.VMEM((blocks, 2, ROWS, LANES), jnp.bfloat16),
            pltpu.VMEM(weight.shape, weight.dtype),
            pltpu.SemaphoreType.DMA((PARTS,)),
        ],
        cost_estimate=pl.CostEstimate(
            flops=2 * depth * blocks * LANES * LANES, bytes_accessed=every.size * 2, transcendentals=0
        ),
        name="statistic",
    )(lags, first, every, power, weight)


def shards(sfts, detector_ids, intersection, lags, template_ids):
    rows, _, bins = sfts.shape
    times = lax.axis_size("tm")
    quarters = lax.axis_size("freq")
    pieces = bins // LANES
    groups = [list(range(g, g + pieces)) for g in range(0, times, pieces)]
    total = detector_ids.shape[0]
    scale = 1.0 / math.sqrt(total * lags.shape[0])
    place = lax.axis_index("tm").astype(jnp.int32)

    send = to_send((place * rows % LANES)[None], sfts, template_ids.T, times)
    every = lax.all_to_all(send, "tm", split_axis=0, concat_axis=0, tiled=True)
    weight = weights(lags, intersection, detector_ids.reshape(total // LANES, LANES))
    every, place, weight = lax.optimization_barrier((every, place, weight))

    power = every[:, 2 * rows : 2 * rows + 3].astype(jnp.float32).sum(axis=1)
    power = lax.all_gather(power, "freq", axis=0, tiled=True).reshape(quarters, *power.shape)
    first = (place // pieces * pieces)[None]
    every = pltpu.with_memory_space_constraint(every, pltpu.VMEM)
    power = pltpu.with_memory_space_constraint(power, pltpu.VMEM)
    part = statistic(lags, first, every, power, weight, pieces, scale, total)
    mine = lax.all_to_all(part, "tm", split_axis=0, concat_axis=0, axis_index_groups=groups, tiled=True)
    return jnp.moveaxis(mine.astype(jnp.float32), 0, 1).reshape(template_ids.shape[0], bins)


def solution(mesh):
    in_specs = (P("tm", None, "freq"), P(), P(), P(), P("tm", None))
    out_specs = P("tm", "freq")
    return jax.shard_map(shards, mesh=mesh, in_specs=in_specs, out_specs=out_specs, check_vma=False)
```

```python
import functools
import math

import jax
import jax.numpy as jnp
from jax import lax
from jax.experimental import pallas as pl
from jax.experimental.pallas import tpu as pltpu
from jax.sharding import PartitionSpec as P

NBIN = 4096
LAGMAX = 16
NGRID = 64
PERIOD = 283
ROWS = 288
EROWS = ROWS + LAGMAX
LANES = 128
PARTS = 2
EXTRA = 8

SIN_COEF = (4.442883014678955, -7.308245658874512, 3.606354236602783, -0.8461116552352905, 0.1098245158791542)
COS_COEF = (1.4142135381698608, -6.978850841522217, 5.739460468292236, -1.883557915687561, 0.3106880187988281)


def horner(coef, y):
    total = coef[-1] * y + coef[-2]
    for value in coef[-3::-1]:
        total = total * y + value
    return total


def sincos_turns(x):
    f = x - jnp.round(x)
    y = f * f
    s = horner(SIN_COEF, y) * f
    c = horner(COS_COEF, y)
    return s * c, 1.0 - s * s


def send_kernel(shift_ref, sfts_ref, ids_ref, out_ref):
    rows = sfts_ref.shape[0]
    pieces = sfts_ref.shape[2] // LANES
    copies = out_ref.shape[0] // pieces
    squares = jnp.zeros((rows, LANES), jnp.float32)
    for c in range(2):
        for v in range(pieces):
            tile = sfts_ref[:, c, v * LANES : (v + 1) * LANES]
            squares = squares + tile * tile
            small = tile.astype(jnp.bfloat16)
            for u in range(copies):
                out_ref[u * pieces + v, c * rows : (c + 1) * rows, :] = small
    square = jnp.concatenate([squares, jnp.zeros((LANES - rows, LANES), jnp.float32)], 0)
    power = jnp.sum(square.T, axis=0, keepdims=True)
    power = pltpu.roll(power, shift_ref[0], 1)
    high = power.astype(jnp.bfloat16)
    rest = power - high.astype(jnp.float32)
    middle = rest.astype(jnp.bfloat16)
    low = (rest - middle.astype(jnp.float32)).astype(jnp.bfloat16)
    ids = ids_ref[...].astype(jnp.float32).astype(jnp.bfloat16)
    spare = jnp.zeros((EXTRA - 5, LANES), jnp.bfloat16)
    extra = jnp.concatenate([high, middle, low, ids, spare], 0)
    for d in range(out_ref.shape[0]):
        out_ref[d, 2 * rows :, :] = extra


def to_send(shift, sfts, ids, times):
    rows = sfts.shape[0]
    vmem = pl.BlockSpec(memory_space=pltpu.VMEM)
    return pl.pallas_call(
        send_kernel,
        out_shape=pltpu.VMEM((times, 2 * rows + EXTRA, LANES), jnp.bfloat16),
        in_specs=[pl.BlockSpec(memory_space=pltpu.SMEM), vmem, vmem],
        out_specs=vmem,
        name="to_send",
    )(shift, sfts, ids)


def spread(line):
    return jnp.broadcast_to(line, (LANES, LANES)).T


def weight_kernel(total, lags_ref, inter_ref, det_ref, out_ref, det, near):
    lag = lags_ref[pl.program_id(0)]

    @pl.when(pl.program_id(0) == 0)
    def _():
        for g in range(total // LANES):
            column = spread(det_ref[g : g + 1, :].astype(jnp.float32))
            det[g * LANES : (g + 1) * LANES, :] = column
            for b in range(3):
                near[b, g * LANES : (g + 1) * LANES, :] = jnp.where(
                    column == 0.0, inter_ref[0, b], jnp.where(column == 1.0, inter_ref[1, b], inter_ref[2, b])
                )
        rest = det.shape[0] - total
        det[total:, :] = jnp.zeros((rest, LANES), jnp.float32)
        for b in range(3):
            near[b, total:, :] = jnp.zeros((rest, LANES), jnp.float32)

    for m in range(out_ref.shape[1]):
        for b in range(ROWS // 16):
            i0 = m * PERIOD + b * 16
            far = det[pl.ds(lag + i0, 16), :]
            out_ref[0, m, b * 16 : b * 16 + 16, :] = jnp.where(
                far == 0.0,
                near[0, i0 : i0 + 16, :],
                jnp.where(far == 1.0, near[1, i0 : i0 + 16, :], near[2, i0 : i0 + 16, :]),
            ).astype(jnp.bfloat16)


def weights(lags, intersection, det):
    total = det.size
    cycles = -(-total // PERIOD)
    smem = pl.BlockSpec(memory_space=pltpu.SMEM)
    length = PERIOD * cycles + ROWS + LAGMAX
    length = -(-length // 32) * 32 + 8
    count = lags.shape[0]
    return pl.pallas_call(
        functools.partial(weight_kernel, total),
        grid=(count,),
        out_shape=jax.ShapeDtypeStruct((count, cycles, ROWS, LANES), jnp.bfloat16),
        in_specs=[smem, smem, pl.BlockSpec(det.shape, lambda l: (0, 0))],
        out_specs=pl.BlockSpec((1, cycles, ROWS, LANES), lambda l: (l, 0, 0, 0)),
        scratch_shapes=[pltpu.VMEM((length, LANES), jnp.float32), pltpu.VMEM((3, length, LANES), jnp.float32)],
        cost_estimate=pl.CostEstimate(
            flops=1000 * count * cycles * ROWS * LANES,
            bytes_accessed=2 * count * cycles * ROWS * LANES,
            transcendentals=0,
        ),
        name="weights",
    )(lags, intersection, det)


def stat_kernel(
    scale,
    total,
    lags_ref,
    first_ref,
    every_ref,
    power_ref,
    weight_hbm,
    out_ref,
    z,
    fold,
    sa,
    ca,
    far,
    near,
    weight,
    sems,
):
    lag_count = lags_ref.shape[0]
    devices, rows, _ = every_ref.shape
    rows = (rows - EXTRA) // 2
    blocks = out_ref.shape[0]
    parts = sems.shape[0]
    group = lag_count // parts
    copies = [
        pltpu.make_async_copy(
            weight_hbm.at[p * group : (p + 1) * group], weight.at[p * group : (p + 1) * group], sems.at[p]
        )
        for p in range(parts)
    ]
    for copy in copies:
        copy.start()

    powers = power_ref[0]
    for q in range(1, power_ref.shape[0]):
        powers = powers + power_ref[q]
    factor_of = lax.rsqrt(powers * (1.0 / NBIN) + 1e-06)
    lane = lax.broadcasted_iota(jnp.int32, (1, LANES), 1)
    for g in range(total // LANES):
        first = g * LANES // rows
        last = (g * LANES + LANES - 1) // rows
        line = factor_of[first : first + 1]
        for d in range(first + 1, last + 1):
            line = jnp.where(lane < d * rows - g * LANES, line, factor_of[d : d + 1])
        column = spread(line)
        for h in range(LANES // 16):
            i0 = g * LANES + h * 16
            d, r = divmod(i0, rows)
            for c in range(2):
                raw = every_ref[d, c * rows + r : c * rows + r + 16, :].astype(jnp.float32)
                z[c, i0 : i0 + 16, :] = raw * column[h * 16 : h * 16 + 16]
    rest = z.shape[1] - total
    for c in range(2):
        z[c, total:, :] = jnp.zeros((rest, LANES), jnp.float32)

    for b in range(EROWS // 16):
        r0 = b * 16
        row = lax.broadcasted_iota(jnp.int32, (16, LANES), 0) + r0
        s, c = sincos_turns(row.astype(jnp.float32) * (1.0 / PERIOD))
        sa[r0 : r0 + 16, :] = s
        ca[r0 : r0 + 16, :] = c

    def exp_block(t, carry):
        ids = every_ref[first_ref[0] + t, 2 * rows : 2 * rows + EXTRA, :].astype(jnp.float32)
        amplitude = (8.0 + 4.0 * ids[3:4]) * (1.0 / (2.0 * math.pi))
        sq, cq = sincos_turns(ids[4:5] * (1.0 / NGRID))
        with_sin = jnp.broadcast_to(amplitude * cq, (16, LANES))
        with_cos = jnp.broadcast_to(amplitude * sq, (16, LANES))
        for b in range(EROWS // 16):
            r0 = b * 16
            s, c = sincos_turns(sa[r0 : r0 + 16, :] * with_sin + ca[r0 : r0 + 16, :] * with_cos)
            far[t, 0, r0 : r0 + 16, :] = c
            far[t, 1, r0 : r0 + 16, :] = s
            if r0 < ROWS:
                near[t, 0, r0 : r0 + 16, :] = c.astype(jnp.bfloat16)
                near[t, 1, r0 : r0 + 16, :] = s.astype(jnp.bfloat16)
        return carry

    lax.fori_loop(0, blocks, exp_block, 0)

    def pair_block(lags_here, cycles, b, carry):
        r0 = pl.multiple_of(b * 16, 16)
        lag = {l: lags_ref[l] for l in lags_here}
        acc = {}
        for m in range(cycles):
            i0 = r0 + PERIOD * m
            a = z[0, pl.ds(i0, 16), :]
            bb = z[1, pl.ds(i0, 16), :]
            for l in lags_here:
                j0 = i0 + lag[l]
                w = weight[l, m, pl.ds(r0, 16), :].astype(jnp.float32)
                c = w * z[0, pl.ds(j0, 16), :]
                d = w * z[1, pl.ds(j0, 16), :]
                re = a * c + bb * d
                im = a * d - bb * c
                acc[l] = (re, im) if m == 0 else (acc[l][0] + re, acc[l][1] + im)
        for l in lags_here:
            for c in range(2):
                fold[b * lag_count + l, c * 16 : c * 16 + 16, :] = acc[l][c]
        return carry

    full = total // PERIOD
    split = -(-(total - full * PERIOD) // 16)
    for p in range(parts):
        copies[p].wait()
        here = range(p * group, (p + 1) * group)
        lax.fori_loop(0, split, functools.partial(pair_block, here, full + 1), 0)
        lax.fori_loop(split, ROWS // 16, functools.partial(pair_block, here, full), 0)
    spans = ROWS // 16
    kept = lax.broadcasted_iota(jnp.int32, (16, LANES), 0) < PERIOD - (spans - 1) * 16
    for l in range(lag_count):
        for c in range(2):
            q = (spans - 1) * lag_count + l
            value = fold[q, c * 16 : c * 16 + 16, :].astype(jnp.float32)
            fold[q, c * 16 : c * 16 + 16, :] = jnp.where(kept, value, 0.0)

    wide = 4
    deep = 256
    lag = [lags_ref[l] for l in range(lag_count)]
    sums = [None] * (blocks // wide)
    for k in range(2 * lag_count * ROWS // deep):
        tile = fold[k * deep // 32 : (k + 1) * deep // 32].reshape(deep, LANES).astype(jnp.bfloat16)
        for n in range(blocks // wide):
            columns = []
            for t in range(n * wide, (n + 1) * wide):
                column = []
                for q in range(k * deep // 32, (k + 1) * deep // 32):
                    b, l = divmod(q, lag_count)
                    r0 = b * 16
                    cr = near[t, 0, r0 : r0 + 16, :]
                    ci = near[t, 1, r0 : r0 + 16, :]
                    fr = far[t, 0, pl.ds(lag[l] + r0, 16), :].astype(jnp.bfloat16)
                    fi = far[t, 1, pl.ds(lag[l] + r0, 16), :].astype(jnp.bfloat16)
                    column += [fr * cr + fi * ci, fi * cr - fr * ci]
                columns.append(jnp.concatenate(column, 0))
            term = lax.dot_general(
                tile,
                jnp.concatenate(columns, 1),
                (((0,), (0,)), ((), ())),
                preferred_element_type=jnp.float32,
            )
            sums[n] = term if k == 0 else sums[n] + term
    for n in range(blocks // wide):
        for h in range(wide):
            out_ref[n * wide + h] = (sums[n][:, h * LANES : (h + 1) * LANES] * scale).T.astype(jnp.bfloat16)


def statistic(lags, first, every, power, weight, blocks, scale, total):
    depth = 2 * lags.shape[0] * ROWS
    reach = PERIOD * (total // PERIOD) + ROWS + LAGMAX
    zrows = -(-reach // 32) * 32 + 16
    smem = pl.BlockSpec(memory_space=pltpu.SMEM)
    vmem = pl.BlockSpec(memory_space=pltpu.VMEM)
    f32 = jnp.float32
    return pl.pallas_call(
        functools.partial(stat_kernel, scale, total),
        out_shape=pltpu.VMEM((blocks, LANES, LANES), jnp.bfloat16),
        in_specs=[smem, smem, vmem, vmem, pl.BlockSpec(memory_space=pl.ANY)],
        out_specs=vmem,
        scratch_shapes=[
            pltpu.VMEM((2, zrows, LANES), f32),
            pltpu.VMEM((depth // 32, 32, LANES), f32),
            pltpu.VMEM((EROWS, LANES), f32),
            pltpu.VMEM((EROWS, LANES), f32),
            pltpu.VMEM((blocks, 2, EROWS, LANES), f32),
            pltpu.VMEM((blocks, 2, ROWS, LANES), jnp.bfloat16),
            pltpu.VMEM(weight.shape, weight.dtype),
            pltpu.SemaphoreType.DMA((PARTS,)),
        ],
        cost_estimate=pl.CostEstimate(
            flops=2 * depth * blocks * LANES * LANES, bytes_accessed=every.size * 2, transcendentals=0
        ),
        name="statistic",
    )(lags, first, every, power, weight)


def place_kernel(tiles_ref, out_ref):
    for v in range(tiles_ref.shape[0]):
        out_ref[:, v * LANES : (v + 1) * LANES] = tiles_ref[v].astype(jnp.float32)


def placed(tiles):
    pieces, rows, _ = tiles.shape
    vmem = pl.BlockSpec(memory_space=pltpu.VMEM)
    return pl.pallas_call(
        place_kernel,
        out_shape=jax.ShapeDtypeStruct((rows, pieces * LANES), jnp.float32),
        in_specs=[vmem],
        out_specs=vmem,
        name="placed",
    )(pltpu.with_memory_space_constraint(tiles, pltpu.VMEM))


def shards(sfts, detector_ids, intersection, lags, template_ids):
    rows, _, bins = sfts.shape
    times = lax.axis_size("tm")
    quarters = lax.axis_size("freq")
    pieces = bins // LANES
    groups = [list(range(g, g + pieces)) for g in range(0, times, pieces)]
    total = detector_ids.shape[0]
    scale = 1.0 / math.sqrt(total * lags.shape[0])
    place = lax.axis_index("tm").astype(jnp.int32)

    send = to_send((place * rows % LANES)[None], sfts, template_ids.T, times)
    every = lax.all_to_all(send, "tm", split_axis=0, concat_axis=0, tiled=True)
    weight = weights(lags, intersection, detector_ids.reshape(total // LANES, LANES))
    every, place, weight = lax.optimization_barrier((every, place, weight))

    power = every[:, 2 * rows : 2 * rows + 3].astype(jnp.float32).sum(axis=1)
    power = lax.all_gather(power, "freq", axis=0, tiled=True).reshape(quarters, *power.shape)
    first = (place // pieces * pieces)[None]
    every = pltpu.with_memory_space_constraint(every, pltpu.VMEM)
    power = pltpu.with_memory_space_constraint(power, pltpu.VMEM)
    part = statistic(lags, first, every, power, weight, pieces, scale, total)
    mine = lax.all_to_all(part, "tm", split_axis=0, concat_axis=0, axis_index_groups=groups, tiled=True)
    return placed(mine)


def solution(mesh):
    in_specs = (P("tm", None, "freq"), P(), P(), P(), P("tm", None))
    out_specs = P("tm", "freq")
    return jax.shard_map(shards, mesh=mesh, in_specs=in_specs, out_specs=out_specs, check_vma=False)
```
